32 devices in a mesh: section: 4 (over y, core), expert: 8 (over z, x).
Axes of the slice: x: 2, y: 2, z: 4, core: 2. Of those that a mesh axis runs over, the one named last changes fastest.
Arguments:
- inputs: bfloat16 [4, 1024, 1024], P('section', 'expert'), may hold values from -6 to 6
- out_grads: bfloat16 [4, 1024, 1024], P('section', 'expert'), may hold values from -6 to 6
- expert_ids: int32 [4, 1024, 8], P('section', 'expert'), may hold values from 0 to 15, all different within a row; in each aligned block of 128 rows (0 to 127, 128 to 255, ..., all dimensions but the last counted through in order) at most 96 rows name the same one
- route_levels: int32 [4, 1024, 8], P('section', 'expert'), may hold values from 8 to 256
- w_gate: bfloat16 [4, 16, 1024, 384], P('section', 'expert'), may hold values from -0.1875 to 0.1875
- w_up: bfloat16 [4, 16, 1024, 384], P('section', 'expert'), may hold values from -0.1875 to 0.1875
- w_down: bfloat16 [4, 16, 384, 1024], P('section', 'expert'), may hold values from -0.3125 to 0.3125
Outputs:
- upstream: bfloat16 [4, 1024, 1024], P('section', 'expert')
- route_grad: bfloat16 [4, 1024, 8], P('section', 'expert')
- gate_update: bfloat16 [4, 16, 1024, 384], P('section', 'expert')
- up_update: bfloat16 [4, 16, 1024, 384], P('section', 'expert')
- down_update: bfloat16 [4, 16, 384, 1024], P('section', 'expert')
The draws below stay inside these ranges and needn't reach their ends.
Inputs may be any that keep to these rules, and one draw needn't show every extreme that they name: `expert_ids`: each token names 8 different experts; among the 128 tokens of one aligned block no expert is named more than 96 times.
All inputs are finite; a program needn't handle non-finite values.
Results may differ from the reference program's by a relative error of at most 0.0064.
Values may be sent and summed in bfloat16 or wider, within the bound.
A program may use at most 128 MiB of HBM per device.

```python
import math
import jax
import jax.numpy as jnp
import numpy as np
from jax import lax

D = 1024
H = 384
TOPK = 8
TOK_DEV = 128
EXPERTS = 16
CAP = 96
SECTIONS = 4
TOKENS = 1024
N_EXPERT = 8


def set_ends(entries, own_key, least, high):
    shape = entries.shape
    index_at = [jax.random.randint(jax.random.fold_in(own_key, axis), (), 0, shape[axis]) for axis in range(len(shape))]
    entries = entries.at[tuple(index_at)].set(least)
    longest = shape.index(max(shape))
    index_at[longest] = (index_at[longest] + 1) % shape[longest]
    return entries.at[tuple(index_at)].set(high)


def block_scale(key, extent, split, least, high):
    factor_of = 1.0
    for position, blocks in split:
        heights = jax.random.uniform(jax.random.fold_in(jax.random.fold_in(key, 6), position), (blocks,), jnp.float32, least / len(split), high / len(split))
        factor_of = factor_of * jnp.repeat(jnp.exp(heights), extent[position] // blocks).reshape((-1,) + (1,) * (len(extent) - 1 - position))
    return factor_of


def routed_block(key, own, number, rows, number_of, top, reach, skew):
    ranking = jax.random.permutation(key, number_of)
    crowded, ordinary = shares(number_of, rows * top, reach, skew, True), shares(number_of, rows * top, reach, skew, False)
    places = jnp.arange(number_of)

    def named(sizes, rotation):
        used = int((sizes > 0).sum())
        fixed = max(1, used // 4)
        moved = fixed + (places - fixed + rotation * (used - fixed)) % max(1, number_of - fixed)
        return jnp.zeros((number_of,), jnp.int32).at[ranking[jnp.where(places < fixed, places, moved)]].set(jnp.asarray(sizes, jnp.int32))

    sizes = jnp.where(number % 4 == 0, named(crowded, number // 4), named(ordinary, number - number // 4 - 1))
    mixed = jax.random.permutation(jax.random.fold_in(own, 3), number_of)
    giver, receiver = mixed[0:number_of // 2 * 2:2], mixed[1:number_of // 2 * 2:2]
    room = jnp.minimum(sizes[giver] - 1, reach - sizes[receiver]) // 2
    room = jnp.where((giver == ranking[0]) | (receiver == ranking[0]) | (sizes[receiver] == 0), 0, jnp.maximum(room, 0))
    moved = jax.random.randint(jax.random.fold_in(own, 4), (number_of // 2,), 0, 1 << 20) % (room + 1)
    sizes = sizes.at[giver].add(-moved).at[receiver].add(moved)
    labels = jnp.searchsorted(jnp.cumsum(sizes), jnp.arange(rows * top), side="right").astype(jnp.int32)
    grid = labels.reshape(top, rows).T
    grid = grid[jax.random.permutation(jax.random.fold_in(own, 1), rows)]
    rotation = jax.random.randint(jax.random.fold_in(own, 2), (rows, 1), 0, top)
    return jnp.take_along_axis(grid, (jnp.arange(top)[None, :] + rotation) % top, axis=1)


def shares(number_of, total, reach, skew, full):
    portions = [(1 << 20) // math.isqrt(rank ** skew) + 1 for rank in range(1, number_of + 1)]
    largest = reach if full else min(reach, max(-(-total // number_of), total * portions[0] // sum(portions)))
    least = 1 if total - largest >= number_of - 1 else 0
    counts, spare = [largest] + [least] * (number_of - 1), total - largest - least * (number_of - 1)
    while spare > 0:
        candidates = [i for i in range(1, number_of) if counts[i] < largest] or [i for i in range(1, number_of) if counts[i] < reach]
        pool, budget = sum([portions[i] for i in candidates]), spare
        for i in candidates:
            extra = min(reach - counts[i], max(1, budget * portions[i] // pool), spare)
            counts[i] = counts[i] + extra
            spare = spare - extra
    return np.array(counts)


def gaussian(own_key, extent, deviation, most, cuts=(), kind=jnp.bfloat16):
    factor_of = block_scale(own_key, extent, cuts, -0.22, 0.18) if cuts else 1.0
    array = jax.random.normal(own_key, extent, jnp.float32) * deviation * factor_of
    return jnp.minimum(jnp.maximum(array, -most), most).astype(kind)


def setup_inputs(seed: int = 0) -> dict:
    keys = jax.random.split(jax.random.key(seed), 8)
    inputs = gaussian(keys[0], (SECTIONS, TOKENS, D), 1.0, 6.0, ((0, 4), (1, 8)))
    out_grads = gaussian(keys[1], (SECTIONS, TOKENS, D), 1.0, 6.0, ((0, 4), (1, 8)))
    expert_ids_keys = jax.random.split(jax.random.fold_in(keys[2], 1), SECTIONS * TOKENS // TOK_DEV)
    expert_ids_turns = jax.random.permutation(jax.random.fold_in(keys[2], 3), SECTIONS * TOKENS // TOK_DEV)
    expert_ids = jax.vmap(lambda own, number: routed_block(jax.random.fold_in(keys[2], 2), own, number, TOK_DEV, EXPERTS, TOPK, CAP, 2))(expert_ids_keys, expert_ids_turns).reshape((SECTIONS, TOKENS, TOPK))
    route_levels = set_ends(jax.random.randint(keys[3], (SECTIONS, TOKENS, TOPK), 8, 257), jax.random.fold_in(keys[3], 1), 8, 256).astype(jnp.int32)
    w_gate = gaussian(keys[4], (SECTIONS, EXPERTS, D, H), D ** -0.5, 0.1875, ((0, 4), (1, 8)))
    w_up = gaussian(keys[5], (SECTIONS, EXPERTS, D, H), D ** -0.5, 0.1875, ((0, 4), (1, 8)))
    w_down = gaussian(keys[6], (SECTIONS, EXPERTS, H, D), H ** -0.5, 0.3125, ((0, 4), (1, 8)))
    return {"inputs": inputs, "out_grads": out_grads, "expert_ids": expert_ids, "route_levels": route_levels, "w_gate": w_gate, "w_up": w_up, "w_down": w_down}


def flat_slots(expert_ids, experts_all, capacity):
    blocks = expert_ids.shape[0]
    flat_ids = expert_ids.reshape(blocks, -1).astype(jnp.int32)
    catalog = jnp.arange(experts_all, dtype=jnp.int32)
    onehot = (flat_ids[:, :, None] == catalog[None, None, :]).astype(jnp.int32)
    rank_table = (jnp.cumsum(onehot, axis=1) - 1).astype(jnp.int32)
    slot_of = jnp.sum(onehot * rank_table, axis=2).astype(jnp.int32)
    return (flat_ids * capacity + slot_of).astype(jnp.int32).reshape(expert_ids.shape)


def expert_backward(slot_inputs, slot_grads, slot_routes, w_gate, w_up, w_down):
    inputs_wide = slot_inputs.astype(jnp.float32)
    grads_wide = slot_grads.astype(jnp.float32)
    gate_wide = w_gate.astype(jnp.float32)
    up_wide = w_up.astype(jnp.float32)
    down_wide = w_down.astype(jnp.float32)
    gate_pre = jnp.einsum('esd,edh->esh', inputs_wide, gate_wide)
    up_pre = jnp.einsum('esd,edh->esh', inputs_wide, up_wide)
    sigmoid_gate = jax.nn.sigmoid(gate_pre)
    silu_gate = gate_pre * sigmoid_gate
    active = (silu_gate * up_pre).astype(jnp.bfloat16)
    active_wide = active.astype(jnp.float32)
    expert_out = jnp.einsum('esh,ehd->esd', active_wide, down_wide)
    route_part = jnp.sum(grads_wide * expert_out, axis=2).astype(jnp.bfloat16)
    weighted = (slot_routes.astype(jnp.float32)[:, :, None] * grads_wide).astype(jnp.bfloat16)
    weighted_wide = weighted.astype(jnp.float32)
    active_grad = jnp.einsum('esd,ehd->esh', weighted_wide, down_wide)
    gate_pre_grad = (active_grad * up_pre * sigmoid_gate * (1.0 + gate_pre * (1.0 - sigmoid_gate))).astype(jnp.bfloat16)
    up_pre_grad = (active_grad * silu_gate).astype(jnp.bfloat16)
    gate_grad_wide = gate_pre_grad.astype(jnp.float32)
    up_grad_wide = up_pre_grad.astype(jnp.float32)
    input_grad = (jnp.einsum('esh,edh->esd', gate_grad_wide, gate_wide)
                  + jnp.einsum('esh,edh->esd', up_grad_wide, up_wide)).astype(jnp.bfloat16)
    down_part = jnp.einsum('esh,esd->ehd', active_wide, weighted_wide).astype(jnp.bfloat16)
    gate_part = jnp.einsum('esd,esh->edh', inputs_wide, gate_grad_wide).astype(jnp.bfloat16)
    up_part = jnp.einsum('esd,esh->edh', inputs_wide, up_grad_wide).astype(jnp.bfloat16)
    return input_grad, route_part, gate_part, up_part, down_part


def section_backward(operands):
    inputs, out_grads, expert_ids, route_levels, w_gate, w_up, w_down = operands
    blocks = N_EXPERT
    flat_index = flat_slots(expert_ids.reshape(blocks, TOK_DEV, TOPK), EXPERTS, CAP)
    catalog = jnp.arange(EXPERTS * CAP, dtype=jnp.int32)
    select = (flat_index[..., None] == catalog).astype(jnp.float32).reshape(blocks, TOK_DEV, TOPK, EXPERTS, CAP)
    placing = jnp.sum(select, axis=2)
    route_values = (route_levels.astype(jnp.float32) / 256.0).reshape(blocks, TOK_DEV, TOPK)
    inputs_wide = inputs.astype(jnp.float32).reshape(blocks, TOK_DEV, D)
    grads_wide = out_grads.astype(jnp.float32).reshape(blocks, TOK_DEV, D)
    slot_inputs = jnp.einsum('btec,btd->ebcd', placing, inputs_wide).reshape(EXPERTS, blocks * CAP, D).astype(jnp.bfloat16)
    slot_grads = jnp.einsum('btec,btd->ebcd', placing, grads_wide).reshape(EXPERTS, blocks * CAP, D).astype(jnp.bfloat16)
    slot_routes = jnp.einsum('btkec,btk->ebc', select, route_values).reshape(EXPERTS, blocks * CAP).astype(jnp.bfloat16)
    input_grad, route_part, gate_part, up_part, down_part = expert_backward(slot_inputs, slot_grads, slot_routes, w_gate, w_up, w_down)
    back_inputs = input_grad.astype(jnp.float32).reshape(EXPERTS, blocks, CAP, D)
    token_grad = jnp.einsum('btec,ebcd->btd', placing, back_inputs).reshape(TOKENS, D).astype(jnp.bfloat16)
    back_routes = route_part.astype(jnp.float32).reshape(EXPERTS, blocks, CAP)
    token_route = jnp.einsum('btkec,ebc->btk', select, back_routes).reshape(TOKENS, TOPK).astype(jnp.bfloat16)
    return token_grad, token_route, gate_part, up_part, down_part


def reference(inputs, out_grads, expert_ids, route_levels, w_gate, w_up, w_down):
    token_grad, token_route, gate_part, up_part, down_part = lax.map(
        section_backward, (inputs, out_grads, expert_ids, route_levels, w_gate, w_up, w_down))
    upstream = jnp.concatenate([token_grad[1:], jnp.zeros_like(token_grad[:1])], axis=0)
    return upstream, token_route, gate_part, up_part, down_part
```

```python
import functools
import math

import jax
import jax.numpy as jnp
from jax import lax
from jax.experimental import pallas as pl
from jax.experimental.pallas import tpu as pltpu
from jax.sharding import PartitionSpec as P

MESH = pl.DeviceIdType.MESH


def kernel(
    lines, rows, sections,
    ids_ref, levels_ref, in_ref, grad_ref, wg_ref, wu_ref, wd_ref,
    up_ref, own_route_ref, gate_ref, up_out_ref, down_ref,
    acts, grads, routes, w_in, w_down, hidden_grads, scaled_all,
    part_out, part_in, back_out, back_in, token,
    load_sem, weight_sem, store_sem,
    z_send, x_send, act_recv, grad_recv, route_send, route_recv,
    part_send, part_recv, back_send, back_recv, y_send, y_recv,
):
    blocks = lines * rows
    tok, width = in_ref.shape
    local, _, hidden = wg_ref.shape
    experts = blocks * local
    me = lax.axis_index("expert")
    section = lax.axis_index("section")
    z, x = me // rows, lax.rem(me, rows)

    def at(line, dx):
        return line * rows + lax.rem(x + dx, rows)

    nearest_end = jnp.minimum(z, lines - 1 - z)
    inward = jnp.where(2 * z < lines, 1, -1)

    def line_at(k):
        both = k <= 2 * nearest_end
        far = jnp.where(both, (k + 1) // 2, k - nearest_end)
        sign = jnp.where(both & (lax.rem(k, 2) == 0), -inward, inward)
        return z + far * sign

    loads = [
        pltpu.make_async_copy(in_ref, acts.at[me], load_sem.at[0]),
        pltpu.make_async_copy(grad_ref, grads.at[me], load_sem.at[1]),
    ]
    weights = []
    for e in range(local):
        weights.append((wg_ref.at[e], w_in.at[:, pl.ds(2 * e * hidden, hidden)]))
        weights.append((wu_ref.at[e], w_in.at[:, pl.ds((2 * e + 1) * hidden, hidden)]))
        weights.append((wd_ref.at[e], w_down.at[pl.ds(e * hidden, hidden), :]))
    weights = [pltpu.make_async_copy(a, b, weight_sem.at[i]) for i, (a, b) in enumerate(weights)]
    for copy in loads + weights:
        copy.start()

    barrier = pltpu.get_barrier_semaphore()
    for d in range(1, blocks):
        pl.semaphore_signal(
            barrier, inc=1, device_id={"expert": lax.rem(me + d, blocks)}, device_id_type=MESH
        )
    before = lax.rem(section + sections - 1, sections)
    after = lax.rem(section + 1, sections)
    for other in (before, after):
        pl.semaphore_signal(barrier, inc=1, device_id={"section": other}, device_id_type=MESH)

    ids = ids_ref[...]
    levels = levels_ref[...]
    expert_row = lax.broadcasted_iota(jnp.int32, (experts, tok), 0)
    mine_routes = jnp.zeros((experts, tok), jnp.float32)
    for k in range(ids.shape[0]):
        level = levels[k : k + 1, :].astype(jnp.float32) * (1.0 / 256.0)
        mine_routes = mine_routes + jnp.where(ids[k : k + 1, :] == expert_row, level, 0.0)
    routes[me] = mine_routes

    pl.semaphore_wait(barrier, blocks + 1)

    halves = ((acts, act_recv), (grads, grad_recv))

    def z_copy(line, side, half):
        buffer, recv = halves[half]
        block = at(line, 0)
        return pltpu.make_async_remote_copy(
            src_ref=buffer.at[block], dst_ref=buffer.at[block],
            send_sem=z_send.at[line, (side + 1) // 2, half], recv_sem=recv.at[block],
            device_id={"expert": me + side * rows}, device_id_type=MESH,
        )

    def x_copy(line, dx, half):
        buffer, recv = halves[half]
        block = at(line, 0)
        return pltpu.make_async_remote_copy(
            src_ref=buffer.at[block], dst_ref=buffer.at[block],
            send_sem=x_send.at[line, dx, half], recv_sem=recv.at[block],
            device_id={"expert": at(z, dx)}, device_id_type=MESH,
        )

    def arrived(block, half):
        buffer, recv = halves[half]
        pltpu.make_async_remote_copy(
            src_ref=buffer.at[block], dst_ref=buffer.at[block],
            send_sem=x_send.at[0, 0, half], recv_sem=recv.at[block],
            device_id={"expert": at(z, 1)}, device_id_type=MESH,
        ).wait_recv()

    def passes(line, side):
        if side > 0:
            return (line <= z) & (z < lines - 1)
        return (line >= z) & (z > 0)

    def forward(line, half):
        for side in (1, -1):
            @pl.when(passes(line, side))
            def _():
                z_copy(line, side, half).start()
        for dx in range(1, rows):
            x_copy(line, dx, half).start()

    def route_copy(d):
        other = lax.rem(me + d, blocks)
        return pltpu.make_async_remote_copy(
            src_ref=routes.at[me], dst_ref=routes.at[me],
            send_sem=route_send.at[d], recv_sem=route_recv.at[me],
            device_id={"expert": other}, device_id_type=MESH,
        )

    def part_copy(block):
        return pltpu.make_async_remote_copy(
            src_ref=part_out.at[block], dst_ref=part_in.at[me],
            send_sem=part_send.at[block], recv_sem=part_recv.at[me],
            device_id={"expert": block}, device_id_type=MESH,
        )

    def back_copy(block):
        return pltpu.make_async_remote_copy(
            src_ref=back_out.at[block], dst_ref=back_in.at[me],
            send_sem=back_send.at[block], recv_sem=back_recv.at[me],
            device_id={"expert": block}, device_id_type=MESH,
        )

    for half in range(2):
        loads[half].wait()
        forward(z, half)
    for d in range(1, blocks):
        route_copy(d).start()
    for copy in weights:
        copy.wait()

    last_dims = (((1,), (1,)), ((), ()))
    first = me * local
    diagonal = lax.broadcasted_iota(jnp.int32, (tok, tok), 0) == lax.broadcasted_iota(
        jnp.int32, (tok, tok), 1
    )
    back_row = lax.broadcasted_iota(jnp.int32, back_out.shape[1:], 0)

    def compute(block):
        pre = jnp.dot(acts[block], w_in[...], preferred_element_type=jnp.float32)
        back_all = lax.dot_general(
            grads[block], w_down[...], last_dims, preferred_element_type=jnp.float32
        )
        block_routes = routes[block]
        route_rows = jnp.zeros(back_out.shape[1:], jnp.float32)
        for e in range(local):
            route = jnp.sum(jnp.where(expert_row == first + e, block_routes, 0.0), axis=0, keepdims=True)
            route = jnp.sum(jnp.where(diagonal, route, 0.0), axis=1, keepdims=True)
            gate = pre[:, 2 * e * hidden : (2 * e + 1) * hidden]
            up = pre[:, (2 * e + 1) * hidden : (2 * e + 2) * hidden]
            back = back_all[:, e * hidden : (e + 1) * hidden]
            sig = jax.nn.sigmoid(gate)
            silu = gate * sig
            active = silu * up
            route_grad = jnp.sum(active * back, axis=1, keepdims=True)
            route_grad = jnp.sum(jnp.where(diagonal, route_grad, 0.0), axis=0, keepdims=True)
            route_rows = route_rows + jnp.where(back_row == e, route_grad, 0.0)
            back = back * route
            hidden_grads[block, :, pl.ds(2 * e * hidden, hidden)] = (
                back * up * sig * (1.0 + gate * (1.0 - sig))
            ).astype(jnp.bfloat16)
            hidden_grads[block, :, pl.ds((2 * e + 1) * hidden, hidden)] = (back * silu).astype(jnp.bfloat16)
            scaled_all[block, :, pl.ds(e * hidden, hidden)] = (active * route).astype(jnp.bfloat16)
        total = lax.dot_general(
            hidden_grads[block], w_in[...], last_dims, preferred_element_type=jnp.float32
        )
        part_out[block] = total.astype(jnp.bfloat16)
        back_out[block] = route_rows

    def step(j, carry):
        after_first = j - 1
        group = jnp.where(j == 0, 0, after_first // rows + 1)
        dx = jnp.where(j == 0, 0, lax.rem(after_first + rows, rows) + jnp.where(group == lines, 1, 0))
        line = line_at(group - jnp.where(dx > 0, 1, 0))
        block = at(line, dx)

        @pl.when((dx == 0) & (j > 0))
        def _():
            for half in range(2):
                arrived(block, half)
                forward(line, half)

        @pl.when(dx > 0)
        def _():
            for half in range(2):
                arrived(block, half)

        @pl.when(j > 0)
        def _():
            pltpu.make_async_remote_copy(
                src_ref=routes.at[block], dst_ref=routes.at[block],
                send_sem=route_send.at[0], recv_sem=route_recv.at[block],
                device_id={"expert": at(z, 1)}, device_id_type=MESH,
            ).wait_recv()

        compute(block)

        @pl.when(j > 0)
        def _():
            part_copy(block).start()
            back_copy(block).start()

        return carry

    lax.fori_loop(0, blocks, step, 0)

    first_dims = (((0,), (0,)), ((), ()))
    all_rows = blocks * tok
    tile = 256 if width % 256 == 0 and (local * hidden) % 256 == 0 else 128

    @pl.loop(0, width // tile)
    def _(c):
        at_c = pl.ds(pl.multiple_of(c * tile, tile), tile)
        left = acts[:, :, at_c].reshape(all_rows, tile)
        right = hidden_grads[...].reshape(all_rows, 2 * local * hidden)
        w_in[at_c, :] = lax.dot_general(
            left, right, first_dims, preferred_element_type=jnp.float32
        ).astype(jnp.bfloat16)

    stores = []
    for e in range(local):
        stores.append((w_in.at[:, pl.ds(2 * e * hidden, hidden)], gate_ref.at[e]))
        stores.append((w_in.at[:, pl.ds((2 * e + 1) * hidden, hidden)], up_out_ref.at[e]))
    for e in range(local):
        stores.append((w_down.at[pl.ds(e * hidden, hidden), :], down_ref.at[e]))
    stores = [pltpu.make_async_copy(a, b, store_sem.at[i]) for i, (a, b) in enumerate(stores)]
    for copy in stores[: 2 * local]:
        copy.start()

    @pl.loop(0, local * hidden // tile)
    def _(c):
        at_c = pl.ds(pl.multiple_of(c * tile, tile), tile)
        left = scaled_all[:, :, at_c].reshape(all_rows, tile)
        right = grads[...].reshape(all_rows, width)
        w_down[at_c, :] = lax.dot_general(
            left, right, first_dims, preferred_element_type=jnp.float32
        ).astype(jnp.bfloat16)

    for copy in stores[2 * local :]:
        copy.start()

    value = part_out[me].astype(jnp.float32)
    for d in range(1, blocks):
        other = lax.rem(me + d, blocks)
        pltpu.make_async_remote_copy(
            src_ref=part_out.at[other], dst_ref=part_in.at[other],
            send_sem=part_send.at[other], recv_sem=part_recv.at[other],
            device_id={"expert": other}, device_id_type=MESH,
        ).wait_recv()
        value = value + part_in[other].astype(jnp.float32)
    token[...] = value.astype(jnp.bfloat16)

    hop = pltpu.make_async_remote_copy(
        src_ref=token, dst_ref=up_ref, send_sem=y_send, recv_sem=y_recv,
        device_id={"section": before}, device_id_type=MESH,
    )

    @pl.when(section > 0)
    def _():
        hop.start()

    @pl.when(section == sections - 1)
    def _():
        up_ref[...] = jnp.zeros_like(up_ref)

    back_in[me] = back_out[me]
    for d in range(1, blocks):
        other = lax.rem(me + d, blocks)
        pltpu.make_async_remote_copy(
            src_ref=back_out.at[other], dst_ref=back_in.at[other],
            send_sem=back_send.at[other], recv_sem=back_recv.at[other],
            device_id={"expert": other}, device_id_type=MESH,
        ).wait_recv()
    route_total = jnp.zeros(ids.shape, jnp.float32)
    for b in range(blocks):
        rows_of = back_in[b]
        for e in range(local):
            route_total = route_total + jnp.where(ids == b * local + e, rows_of[e : e + 1, :], 0.0)
    own_route_ref[...] = route_total.astype(jnp.bfloat16)

    for line in range(lines):
        for half in range(2):
            for side in (1, -1):
                @pl.when(passes(line, side))
                def _():
                    z_copy(line, side, half).wait_send()
            for dx in range(1, rows):
                x_copy(line, dx, half).wait_send()
    for d in range(1, blocks):
        other = lax.rem(me + d, blocks)
        route_copy(d).wait_send()
        part_copy(other).wait_send()
        back_copy(other).wait_send()

    @pl.when(section > 0)
    def _():
        hop.wait_send()

    @pl.when(section < sections - 1)
    def _():
        hop.wait_recv()

    for copy in stores:
        copy.wait()


def body(rows, inputs, out_grads, expert_ids, route_levels, w_gate, w_up, w_down):
    tok, width = inputs.shape[1:]
    local, _, hidden = w_gate.shape[1:]
    blocks = lax.axis_size("expert")
    sections = lax.axis_size("section")
    lines = blocks // rows
    experts = blocks * local
    top = expert_ids.shape[2]
    bf16 = jnp.bfloat16
    f32 = jnp.float32
    anywhere = pl.BlockSpec(memory_space=pl.ANY)
    inside = pl.BlockSpec(memory_space=pltpu.VMEM)
    dma = pltpu.SemaphoreType.DMA
    back_rows = -(-local // 8) * 8
    upstream, own_routes, gates, ups, downs = pl.pallas_call(
        functools.partial(kernel, lines, rows, sections),
        out_shape=(
            jax.ShapeDtypeStruct((tok, width), bf16),
            jax.ShapeDtypeStruct((top, tok), bf16),
            jax.ShapeDtypeStruct(w_gate.shape[1:], bf16),
            jax.ShapeDtypeStruct(w_up.shape[1:], bf16),
            jax.ShapeDtypeStruct(w_down.shape[1:], bf16),
        ),
        in_specs=[inside] * 2 + [anywhere] * 5,
        out_specs=(inside, inside, anywhere, anywhere, anywhere),
        scratch_shapes=[
            pltpu.VMEM((blocks, tok, width), bf16),
            pltpu.VMEM((blocks, tok, width), bf16),
            pltpu.VMEM((blocks, experts, tok), f32),
            pltpu.VMEM((width, 2 * local * hidden), bf16),
            pltpu.VMEM((local * hidden, width), bf16),
            pltpu.VMEM((blocks, tok, 2 * local * hidden), bf16),
            pltpu.VMEM((blocks, tok, local * hidden), bf16),
            pltpu.VMEM((blocks, tok, width), bf16),
            pltpu.VMEM((blocks, tok, width), bf16),
            pltpu.VMEM((blocks, back_rows, tok), f32),
            pltpu.VMEM((blocks, back_rows, tok), f32),
            pltpu.VMEM((tok, width), bf16),
            dma((2,)),
            dma((3 * local,)),
            dma((3 * local,)),
            dma((lines, 2, 2)),
            dma((lines, rows, 2)),
            dma((blocks,)),
            dma((blocks,)),
            dma((blocks,)),
            dma((blocks,)),
            dma((blocks,)),
            dma((blocks,)),
            dma((blocks,)),
            dma((blocks,)),
            dma,
            dma,
        ],
        compiler_params=pltpu.CompilerParams(
            collective_id=0, has_side_effects=True, vmem_limit_bytes=66_000_000
        ),
    )(
        jnp.swapaxes(expert_ids[0], 0, 1), jnp.swapaxes(route_levels[0], 0, 1),
        inputs[0], out_grads[0], w_gate[0], w_up[0], w_down[0],
    )
    token_route = jnp.swapaxes(own_routes, 0, 1)
    return (upstream[None], token_route[None], gates[None], ups[None], downs[None])


def solution(mesh):
    blocks = mesh.shape["expert"]
    rows = math.isqrt(max(blocks // 2, 1))
    while blocks % rows:
        rows -= 1
    in_specs = (
        P("section", "expert", None),
        P("section", "expert", None),
        P("section", "expert", None),
        P("section", "expert", None),
        P("section", "expert", None, None),
        P("section", "expert", None, None),
        P("section", "expert", None, None),
    )
    out_specs = (
        P("section", "expert", None),
        P("section", "expert", None),
        P("section", "expert", None, None),
        P("section", "expert", None, None),
        P("section", "expert", None, None),
    )
    return jax.shard_map(
        functools.partial(body, rows), mesh=mesh, in_specs=in_specs, out_specs=out_specs, check_vma=False
    )
```

```python
import functools
import math

import jax
import jax.numpy as jnp
from jax import lax
from jax.experimental import pallas as pl
from jax.experimental.pallas import tpu as pltpu
from jax.sharding import PartitionSpec as P

MESH = pl.DeviceIdType.MESH
COLUMN = (1,)
STRAIGHT = ()
CUTS = 2


def kernel(
    lines, rows, sections,
    ids_ref, levels_ref, in_ref, grad_ref, wg_ref, wu_ref, wd_ref,
    up_ref, own_route_ref, gate_ref, up_out_ref, down_ref,
    acts, grads, routes, w_in, w_down, hidden_grads, scaled_all,
    col_out, col_in, side_out, side_in, back_out, back_in, token, total_ref,
    load_sem, weight_sem,
    z_send, x_send, act_recv, grad_recv, route_send, route_recv,
    col_send, col_recv, side_send, side_recv, back_send, back_recv, y_send, y_recv,
):
    blocks = lines * rows
    tok, width = in_ref.shape
    local, _, hidden = wg_ref.shape
    experts = blocks * local
    me = lax.axis_index("expert")
    section = lax.axis_index("section")
    z, x = me // rows, lax.rem(me, rows)

    def at(line, dx):
        return line * rows + lax.rem(x + dx, rows)

    nearest_end = jnp.minimum(z, lines - 1 - z)
    inward = jnp.where(2 * z < lines, 1, -1)

    def line_at(k):
        both = k <= 2 * nearest_end
        far = jnp.where(both, (k + 1) // 2, k - nearest_end)
        sign = jnp.where(both & (lax.rem(k, 2) == 0), -inward, inward)
        return z + far * sign

    loads = [
        pltpu.make_async_copy(in_ref, acts.at[me], load_sem.at[0]),
        pltpu.make_async_copy(grad_ref, grads.at[me], load_sem.at[1]),
    ]
    weights = []
    for e in range(local):
        weights.append((wg_ref.at[e], w_in.at[:, pl.ds(2 * e * hidden, hidden)]))
        weights.append((wu_ref.at[e], w_in.at[:, pl.ds((2 * e + 1) * hidden, hidden)]))
        weights.append((wd_ref.at[e], w_down.at[pl.ds(e * hidden, hidden), :]))
    weights = [pltpu.make_async_copy(a, b, weight_sem.at[i]) for i, (a, b) in enumerate(weights)]
    for copy in loads + weights:
        copy.start()

    barrier = pltpu.get_barrier_semaphore()
    for d in range(1, blocks):
        pl.semaphore_signal(
            barrier, inc=1, device_id={"expert": lax.rem(me + d, blocks)}, device_id_type=MESH
        )
    before = lax.rem(section + sections - 1, sections)
    after = lax.rem(section + 1, sections)
    for other in (before, after):
        pl.semaphore_signal(barrier, inc=1, device_id={"section": other}, device_id_type=MESH)

    ids = ids_ref[...]
    levels = levels_ref[...]
    expert_row = lax.broadcasted_iota(jnp.int32, (experts, tok), 0)
    mine_routes = jnp.zeros((experts, tok), jnp.float32)
    for k in range(ids.shape[0]):
        level = levels[k : k + 1, :].astype(jnp.float32) * (1.0 / 256.0)
        mine_routes = mine_routes + jnp.where(ids[k : k + 1, :] == expert_row, level, 0.0)
    routes[me] = mine_routes

    pl.semaphore_wait(barrier, blocks + 1)

    halves = ((acts, act_recv), (grads, grad_recv))

    def z_copy(line, side, half):
        buffer, recv = halves[half]
        block = at(line, 0)
        return pltpu.make_async_remote_copy(
            src_ref=buffer.at[block], dst_ref=buffer.at[block],
            send_sem=z_send.at[line, (side + 1) // 2, half], recv_sem=recv.at[block],
            device_id={"expert": me + side * rows}, device_id_type=MESH,
        )

    def x_copy(line, dx, half):
        buffer, recv = halves[half]
        block = at(line, 0)
        return pltpu.make_async_remote_copy(
            src_ref=buffer.at[block], dst_ref=buffer.at[block],
            send_sem=x_send.at[line, dx, half], recv_sem=recv.at[block],
            device_id={"expert": at(z, dx)}, device_id_type=MESH,
        )

    def arrived(block, half):
        buffer, recv = halves[half]
        pltpu.make_async_remote_copy(
            src_ref=buffer.at[block], dst_ref=buffer.at[block],
            send_sem=x_send.at[0, 0, half], recv_sem=recv.at[block],
            device_id={"expert": at(z, 1)}, device_id_type=MESH,
        ).wait_recv()

    def passes(line, side):
        if side > 0:
            return (line <= z) & (z < lines - 1)
        return (line >= z) & (z > 0)

    def forward(line, half):
        for side in (1, -1):
            @pl.when(passes(line, side))
            def _():
                z_copy(line, side, half).start()
        for dx in range(1, rows):
            x_copy(line, dx, half).start()

    def route_copy(d):
        other = lax.rem(me + d, blocks)
        return pltpu.make_async_remote_copy(
            src_ref=routes.at[me], dst_ref=routes.at[me],
            send_sem=route_send.at[d], recv_sem=route_recv.at[me],
            device_id={"expert": other}, device_id_type=MESH,
        )

    def away(line):
        return jnp.abs(line - z)

    def among(line, distances):
        return functools.reduce(jnp.logical_or, [away(line) == d for d in distances], line != line)

    def by_side(line):
        return (line != z) & ~among(line, COLUMN) & ~among(line, STRAIGHT)

    cut_rows = tok // CUTS
    cuts = [pl.ds(c * cut_rows, cut_rows) for c in range(CUTS)]

    def col_copy(line, c):
        return pltpu.make_async_remote_copy(
            src_ref=col_out.at[line, cuts[c]], dst_ref=col_in.at[z, cuts[c]],
            send_sem=col_send.at[line, c], recv_sem=col_recv.at[z, c],
            device_id={"expert": at(line, 0)}, device_id_type=MESH,
        )

    def side_copy(line, dx, slot, target, c):
        return pltpu.make_async_remote_copy(
            src_ref=side_out.at[line, dx - 1, cuts[c]], dst_ref=side_in.at[slot, dx - 1, cuts[c]],
            send_sem=side_send.at[line, dx - 1, c], recv_sem=side_recv.at[slot, dx - 1, c],
            device_id={"expert": target}, device_id_type=MESH,
        )

    def start_col(line):
        @pl.when((line != z) & ~by_side(line))
        def _():
            for c in range(CUTS):
                col_copy(line, c).start()

    def start_side(line, dx):
        for c in range(CUTS):
            @pl.when(by_side(line))
            def _():
                side_copy(line, dx, line, at(z, dx), c).start()

            @pl.when(among(line, COLUMN))
            def _():
                side_copy(line, dx, z, at(line, 0), c).start()

            @pl.when(among(line, STRAIGHT))
            def _():
                side_copy(line, dx, z, at(line, dx), c).start()

    def back_copy(block):
        return pltpu.make_async_remote_copy(
            src_ref=back_out.at[block], dst_ref=back_in.at[me],
            send_sem=back_send.at[block], recv_sem=back_recv.at[me],
            device_id={"expert": block}, device_id_type=MESH,
        )

    for half in range(2):
        loads[half].wait()
        forward(z, half)
    for d in range(1, blocks):
        route_copy(d).start()
    for copy in weights:
        copy.wait()

    last_dims = (((1,), (1,)), ((), ()))
    first = me * local
    diagonal = lax.broadcasted_iota(jnp.int32, (tok, tok), 0) == lax.broadcasted_iota(
        jnp.int32, (tok, tok), 1
    )
    back_row = lax.broadcasted_iota(jnp.int32, back_out.shape[1:], 0)

    def compute(block):
        pre = jnp.dot(acts[block], w_in[...], preferred_element_type=jnp.float32)
        back_all = lax.dot_general(
            grads[block], w_down[...], last_dims, preferred_element_type=jnp.float32
        )
        block_routes = routes[block]
        route_rows = jnp.zeros(back_out.shape[1:], jnp.float32)
        for e in range(local):
            route = jnp.sum(jnp.where(expert_row == first + e, block_routes, 0.0), axis=0, keepdims=True)
            route = jnp.sum(jnp.where(diagonal, route, 0.0), axis=1, keepdims=True)
            gate = pre[:, 2 * e * hidden : (2 * e + 1) * hidden]
            up = pre[:, (2 * e + 1) * hidden : (2 * e + 2) * hidden]
            back = back_all[:, e * hidden : (e + 1) * hidden]
            sig = jax.nn.sigmoid(gate)
            silu = gate * sig
            active = silu * up
            route_grad = jnp.sum(active * back, axis=1, keepdims=True)
            route_grad = jnp.sum(jnp.where(diagonal, route_grad, 0.0), axis=0, keepdims=True)
            route_rows = route_rows + jnp.where(back_row == e, route_grad, 0.0)
            back = back * route
            hidden_grads[block, :, pl.ds(2 * e * hidden, hidden)] = (
                back * up * sig * (1.0 + gate * (1.0 - sig))
            ).astype(jnp.bfloat16)
            hidden_grads[block, :, pl.ds((2 * e + 1) * hidden, hidden)] = (back * silu).astype(jnp.bfloat16)
            scaled_all[block, :, pl.ds(e * hidden, hidden)] = (active * route).astype(jnp.bfloat16)
        total = lax.dot_general(
            hidden_grads[block], w_in[...], last_dims, preferred_element_type=jnp.float32
        )
        back_out[block] = route_rows
        return total.astype(jnp.bfloat16)

    def step(j, carry):
        after_first = j - 1
        group = jnp.where(j == 0, 0, after_first // rows + 1)
        dx = jnp.where(j == 0, 0, lax.rem(after_first + rows, rows) + jnp.where(group == lines, 1, 0))
        line = line_at(group - jnp.where(dx > 0, 1, 0))
        block = at(line, dx)

        @pl.when((dx == 0) & (j > 0))
        def _():
            for half in range(2):
                arrived(block, half)
                forward(line, half)

        last_forward = (lines - 2) * rows + 1

        @pl.when(j == last_forward)
        def _():
            for k in range(1, lines - 1):
                start_col(line_at(k))
            for k in range(1, lines - 2):
                for other in range(1, rows):
                    start_side(line_at(k), other)

        @pl.when(dx > 0)
        def _():
            for half in range(2):
                arrived(block, half)

        @pl.when(j > 0)
        def _():
            pltpu.make_async_remote_copy(
                src_ref=routes.at[block], dst_ref=routes.at[block],
                send_sem=route_send.at[0], recv_sem=route_recv.at[block],
                device_id={"expert": at(z, 1)}, device_id_type=MESH,
            ).wait_recv()

        total = compute(block)

        @pl.when(j > 0)
        def _():
            back_copy(block).start()

        @pl.when(dx == 0)
        def _():
            col_out[line] = total

            @pl.when(j >= last_forward)
            def _():
                start_col(line)

        @pl.when(dx > 0)
        def _():
            side_out[line, dx - 1] = total

            @pl.when(j >= last_forward)
            def _():
                start_side(line, dx)

        return carry

    lax.fori_loop(0, blocks, step, 0)

    def side_arrived(line, dx, c):
        side_copy(line, dx, line, at(z, 1), c).wait_recv()

    for c in range(CUTS):
        for k in range(1, lines):
            line = line_at(k)

            @pl.when(by_side(line))
            def _():
                value = col_out[line, cuts[c]].astype(jnp.float32)
                for dx in range(1, rows):
                    side_arrived(line, dx, c)
                    value = value + side_in[line, dx - 1, cuts[c]].astype(jnp.float32)
                col_out[line, cuts[c]] = value.astype(jnp.bfloat16)
                col_copy(line, c).start()

        for dx in range(1, rows):
            for line in range(lines):
                @pl.when(among(line, COLUMN))
                def _():
                    side_arrived(line, dx, c)
                    side_out[z, dx - 1, cuts[c]] = (
                        side_out[z, dx - 1, cuts[c]].astype(jnp.float32)
                        + side_in[line, dx - 1, cuts[c]].astype(jnp.float32)
                    ).astype(jnp.bfloat16)
            side_copy(z, dx, z, at(z, dx), c).start()

    first_dims = (((0,), (0,)), ((), ()))
    all_rows = blocks * tok
    tile = 256 if width % 256 == 0 and (local * hidden) % 256 == 0 else 128

    @pl.loop(0, width // tile)
    def _(c):
        at_c = pl.ds(pl.multiple_of(c * tile, tile), tile)
        left = acts[:, :, at_c].reshape(all_rows, tile)
        right = hidden_grads[...].reshape(all_rows, 2 * local * hidden)
        update = lax.dot_general(
            left, right, first_dims, preferred_element_type=jnp.float32
        ).astype(jnp.bfloat16)
        for e in range(local):
            gate_ref[e, at_c, :] = update[:, 2 * e * hidden : (2 * e + 1) * hidden]
            up_out_ref[e, at_c, :] = update[:, (2 * e + 1) * hidden : (2 * e + 2) * hidden]

    down_tile = 128
    for e in range(local):
        @pl.loop(0, hidden // down_tile)
        def _(c):
            at_left = pl.ds(pl.multiple_of(e * hidden + c * down_tile, down_tile), down_tile)
            at_c = pl.ds(pl.multiple_of(c * down_tile, down_tile), down_tile)
            left = scaled_all[:, :, at_left].reshape(all_rows, down_tile)
            right = grads[...].reshape(all_rows, width)
            down_ref[e, at_c, :] = lax.dot_general(
                left, right, first_dims, preferred_element_type=jnp.float32
            ).astype(jnp.bfloat16)

    def hop(c):
        return pltpu.make_async_remote_copy(
            src_ref=token.at[cuts[c]], dst_ref=up_ref.at[cuts[c]], send_sem=y_send.at[c], recv_sem=y_recv.at[c],
            device_id={"section": before}, device_id_type=MESH,
        )

    @pl.when(section == sections - 1)
    def _():
        up_ref[...] = jnp.zeros_like(up_ref)

    for c in range(CUTS):
        total_ref[...] = col_out[z, cuts[c]].astype(jnp.float32)

        def take(piece):
            total_ref[...] = total_ref[...] + piece.astype(jnp.float32)

        for line in range(lines):
            @pl.when(line != z)
            def _():
                pltpu.make_async_remote_copy(
                    src_ref=col_out.at[line, cuts[c]], dst_ref=col_in.at[line, cuts[c]],
                    send_sem=col_send.at[line, c], recv_sem=col_recv.at[line, c],
                    device_id={"expert": at(line, 0)}, device_id_type=MESH,
                ).wait_recv()
                take(col_in[line, cuts[c]])

            @pl.when((line == z) | among(line, STRAIGHT))
            def _():
                for dx in range(1, rows):
                    side_arrived(line, dx, c)
                    take(side_in[line, dx - 1, cuts[c]])

        token[cuts[c], :] = total_ref[...].astype(jnp.bfloat16)

        @pl.when(section > 0)
        def _():
            hop(c).start()

    back_in[me] = back_out[me]
    for d in range(1, blocks):
        other = lax.rem(me + d, blocks)
        pltpu.make_async_remote_copy(
            src_ref=back_out.at[other], dst_ref=back_in.at[other],
            send_sem=back_send.at[other], recv_sem=back_recv.at[other],
            device_id={"expert": other}, device_id_type=MESH,
        ).wait_recv()
    route_total = jnp.zeros(ids.shape, jnp.float32)
    for b in range(blocks):
        rows_of = back_in[b]
        for e in range(local):
            route_total = route_total + jnp.where(ids == b * local + e, rows_of[e : e + 1, :], 0.0)
    own_route_ref[...] = route_total.astype(jnp.bfloat16)

    for line in range(lines):
        for half in range(2):
            for side in (1, -1):
                @pl.when(passes(line, side))
                def _():
                    z_copy(line, side, half).wait_send()
            for dx in range(1, rows):
                x_copy(line, dx, half).wait_send()
    for d in range(1, blocks):
        other = lax.rem(me + d, blocks)
        route_copy(d).wait_send()
        back_copy(other).wait_send()
    for line in range(lines):
        @pl.when(line != z)
        def _():
            for c in range(CUTS):
                col_copy(line, c).wait_send()

        for dx in range(1, rows):
            for c in range(CUTS):
                side_copy(line, dx, z, at(z, dx), c).wait_send()

    for c in range(CUTS):
        @pl.when(section > 0)
        def _():
            hop(c).wait_send()

        @pl.when(section < sections - 1)
        def _():
            hop(c).wait_recv()


def finish(*refs):
    sources, targets, sem = refs[:5], refs[5:10], refs[10]
    copies = [pltpu.make_async_copy(a, b, sem.at[i]) for i, (a, b) in enumerate(zip(sources, targets))]
    for copy in copies:
        copy.start()
    for copy in copies:
        copy.wait()


def body(rows, inputs, out_grads, expert_ids, route_levels, w_gate, w_up, w_down):
    tok, width = inputs.shape[1:]
    local, _, hidden = w_gate.shape[1:]
    blocks = lax.axis_size("expert")
    sections = lax.axis_size("section")
    lines = blocks // rows
    experts = blocks * local
    top = expert_ids.shape[2]
    bf16 = jnp.bfloat16
    f32 = jnp.float32
    anywhere = pl.BlockSpec(memory_space=pl.ANY)
    inside = pl.BlockSpec(memory_space=pltpu.VMEM)
    dma = pltpu.SemaphoreType.DMA
    side = max(rows - 1, 1)
    back_rows = -(-local // 8) * 8
    shapes = ((tok, width), (top, tok), w_gate.shape[1:], w_up.shape[1:], w_down.shape[1:])
    limit = 66_900_000 - 2 * sum(-(-math.prod(shape) // 4096) * 4096 for shape in shapes)
    results = pl.pallas_call(
        functools.partial(kernel, lines, rows, sections),
        out_shape=tuple(pltpu.VMEM(shape, bf16) for shape in shapes),
        in_specs=[inside] * 2 + [anywhere] * 5,
        out_specs=(inside,) * 5,
        scratch_shapes=[
            pltpu.VMEM((blocks, tok, width), bf16),
            pltpu.VMEM((blocks, tok, width), bf16),
            pltpu.VMEM((blocks, experts, tok), f32),
            pltpu.VMEM((width, 2 * local * hidden), bf16),
            pltpu.VMEM((local * hidden, width), bf16),
            pltpu.VMEM((blocks, tok, 2 * local * hidden), bf16),
            pltpu.VMEM((blocks, tok, local * hidden), bf16),
            pltpu.VMEM((lines, tok, width), bf16),
            pltpu.VMEM((lines, tok, width), bf16),
            pltpu.VMEM((lines, side, tok, width), bf16),
            pltpu.VMEM((lines, side, tok, width), bf16),
            pltpu.VMEM((blocks, back_rows, tok), f32),
            pltpu.VMEM((blocks, back_rows, tok), f32),
            pltpu.VMEM((tok, width), bf16),
            pltpu.VMEM((tok // CUTS, width), f32),
            dma((2,)),
            dma((3 * local,)),
            dma((lines, 2, 2)),
            dma((lines, rows, 2)),
            dma((blocks,)),
            dma((blocks,)),
            dma((blocks,)),
            dma((blocks,)),
            dma((lines, CUTS)),
            dma((lines, CUTS)),
            dma((lines, side, CUTS)),
            dma((lines, side, CUTS)),
            dma((blocks,)),
            dma((blocks,)),
            dma((CUTS,)),
            dma((CUTS,)),
        ],
        compiler_params=pltpu.CompilerParams(
            collective_id=0, has_side_effects=True, vmem_limit_bytes=limit
        ),
    )(
        jnp.swapaxes(expert_ids[0], 0, 1), jnp.swapaxes(route_levels[0], 0, 1),
        inputs[0], out_grads[0], w_gate[0], w_up[0], w_down[0],
    )
    upstream, own_routes, gates, ups, downs = pl.pallas_call(
        finish,
        out_shape=tuple(jax.ShapeDtypeStruct(shape, bf16) for shape in shapes),
        in_specs=[inside] * 5,
        out_specs=(anywhere,) * 5,
        scratch_shapes=[dma((5,))],
        compiler_params=pltpu.CompilerParams(vmem_limit_bytes=1_000_000),
    )(*[pltpu.with_memory_space_constraint(r, pltpu.VMEM) for r in results])
    token_route = jnp.swapaxes(own_routes, 0, 1)
    return (upstream[None], token_route[None], gates[None], ups[None], downs[None])


def solution(mesh):
    blocks = mesh.shape["expert"]
    rows = math.isqrt(max(blocks // 2, 1))
    while blocks % rows:
        rows -= 1
    in_specs = (
        P("section", "expert", None),
        P("section", "expert", None),
        P("section", "expert", None),
        P("section", "expert", None),
        P("section", "expert", None, None),
        P("section", "expert", None, None),
        P("section", "expert", None, None),
    )
    out_specs = (
        P("section", "expert", None),
        P("section", "expert", None),
        P("section", "expert", None, None),
        P("section", "expert", None, None),
        P("section", "expert", None, None),
    )
    return jax.shard_map(
        functools.partial(body, rows), mesh=mesh, in_specs=in_specs, out_specs=out_specs, check_vma=False
    )
```

```python
import functools
import math

import jax
import jax.numpy as jnp
from jax import lax
from jax.experimental import pallas as pl
from jax.experimental.pallas import tpu as pltpu
from jax.sharding import PartitionSpec as P

MESH = pl.DeviceIdType.MESH
COLUMN = ((1,), (1,))
CUTS = len(COLUMN)


def kernel(
    lines, rows, sections,
    ids_ref, levels_ref, in_ref, grad_ref, wg_ref, wu_ref, wd_ref,
    up_ref, own_route_ref, gate_ref, up_out_ref, down_ref,
    acts, grads, routes, w_in, w_down, hidden_grads, scaled_all,
    col_out, col_in, side_out, side_in, back_out, back_in, ids_in, levels_in,
    small_sem, load_sem, weight_sem,
    z_send, x_send, act_recv, grad_recv, route_send, route_recv,
    col_send, col_recv, side_send, side_recv, back_send, back_recv,
):
    blocks = lines * rows
    tok, width = in_ref.shape
    local, _, hidden = wg_ref.shape
    experts = blocks * local
    me = lax.axis_index("expert")
    section = lax.axis_index("section")
    z, x = me // rows, lax.rem(me, rows)

    def at(line, dx):
        return line * rows + lax.rem(x + dx, rows)

    nearest_end = jnp.minimum(z, lines - 1 - z)
    inward = jnp.where(2 * z < lines, 1, -1)

    def line_at(k):
        both = k <= 2 * nearest_end
        far = jnp.where(both, (k + 1) // 2, k - nearest_end)
        sign = jnp.where(both & (lax.rem(k, 2) == 0), -inward, inward)
        return z + far * sign

    small = [
        pltpu.make_async_copy(ids_ref, ids_in, small_sem.at[0]),
        pltpu.make_async_copy(levels_ref, levels_in, small_sem.at[1]),
    ]
    for copy in small:
        copy.start()
    loads = [
        pltpu.make_async_copy(in_ref, acts.at[me], load_sem.at[0]),
        pltpu.make_async_copy(grad_ref, grads.at[me], load_sem.at[1]),
    ]
    weights = []
    for e in range(local):
        weights.append((wg_ref.at[e], w_in.at[:, pl.ds(2 * e * hidden, hidden)]))
        weights.append((wu_ref.at[e], w_in.at[:, pl.ds((2 * e + 1) * hidden, hidden)]))
        weights.append((wd_ref.at[e], w_down.at[pl.ds(e * hidden, hidden), :]))
    weights = [pltpu.make_async_copy(a, b, weight_sem.at[i]) for i, (a, b) in enumerate(weights)]
    for copy in loads + weights:
        copy.start()

    barrier = pltpu.get_barrier_semaphore()
    for d in range(1, blocks):
        pl.semaphore_signal(
            barrier, inc=1, device_id={"expert": lax.rem(me + d, blocks)}, device_id_type=MESH
        )
    before = lax.rem(section + sections - 1, sections)
    after = lax.rem(section + 1, sections)
    for dz in range(lines):
        line = lax.rem(z + dz, lines)
        for dx in range(rows if dz == 0 else 1):
            pl.semaphore_signal(
                barrier, inc=1, device_id={"expert": at(line, dx), "section": after}, device_id_type=MESH
            )

    for copy in small:
        copy.wait()
    ids = ids_in[...]
    levels = levels_in[...]
    expert_row = lax.broadcasted_iota(jnp.int32, (experts, tok), 0)
    mine_routes = jnp.zeros((experts, tok), jnp.float32)
    for k in range(ids.shape[0]):
        level = levels[k : k + 1, :].astype(jnp.float32) * (1.0 / 256.0)
        mine_routes = mine_routes + jnp.where(ids[k : k + 1, :] == expert_row, level, 0.0)
    routes[me] = mine_routes

    pl.semaphore_wait(barrier, blocks - 1 + lines + rows - 1)

    halves = ((acts, act_recv), (grads, grad_recv))

    def z_copy(line, side, half):
        buffer, recv = halves[half]
        block = at(line, 0)
        return pltpu.make_async_remote_copy(
            src_ref=buffer.at[block], dst_ref=buffer.at[block],
            send_sem=z_send.at[line, (side + 1) // 2, half], recv_sem=recv.at[block],
            device_id={"expert": me + side * rows}, device_id_type=MESH,
        )

    def x_copy(line, dx, half):
        buffer, recv = halves[half]
        block = at(line, 0)
        return pltpu.make_async_remote_copy(
            src_ref=buffer.at[block], dst_ref=buffer.at[block],
            send_sem=x_send.at[line, dx, half], recv_sem=recv.at[block],
            device_id={"expert": at(z, dx)}, device_id_type=MESH,
        )

    def arrived(block, half):
        buffer, recv = halves[half]
        pltpu.make_async_remote_copy(
            src_ref=buffer.at[block], dst_ref=buffer.at[block],
            send_sem=x_send.at[0, 0, half], recv_sem=recv.at[block],
            device_id={"expert": at(z, 1)}, device_id_type=MESH,
        ).wait_recv()

    def passes(line, side):
        if side > 0:
            return (line <= z) & (z < lines - 1)
        return (line >= z) & (z > 0)

    def forward(line, half):
        for side in (1, -1):
            @pl.when(passes(line, side))
            def _():
                z_copy(line, side, half).start()
        for dx in range(1, rows):
            x_copy(line, dx, half).start()

    def route_copy(d):
        other = lax.rem(me + d, blocks)
        return pltpu.make_async_remote_copy(
            src_ref=routes.at[me], dst_ref=routes.at[me],
            send_sem=route_send.at[d], recv_sem=route_recv.at[me],
            device_id={"expert": other}, device_id_type=MESH,
        )

    def away(line):
        return jnp.abs(line - z)

    def among(line, distances):
        return functools.reduce(jnp.logical_or, [away(line) == d for d in distances], line != line)

    def by_side(line, c):
        return (line != z) & ~among(line, COLUMN[c])

    cut_rows = tok // CUTS
    cuts = [pl.ds(c * cut_rows, cut_rows) for c in range(CUTS)]

    def col_copy(line, c):
        return pltpu.make_async_remote_copy(
            src_ref=col_out.at[line, cuts[c]], dst_ref=col_in.at[z, cuts[c]],
            send_sem=col_send.at[line, c], recv_sem=col_recv.at[z, c],
            device_id={"expert": at(line, 0), "section": before}, device_id_type=MESH,
        )

    def side_copy(line, dx, slot, target, c, home=None):
        return pltpu.make_async_remote_copy(
            src_ref=side_out.at[line, dx - 1, cuts[c]], dst_ref=side_in.at[slot, dx - 1, cuts[c]],
            send_sem=side_send.at[line, dx - 1, c], recv_sem=side_recv.at[slot, dx - 1, c],
            device_id={"expert": target, "section": section if home is None else home},
            device_id_type=MESH,
        )

    def start_col(line):
        for c in range(CUTS):
            @pl.when(~by_side(line, c))
            def _():
                col_copy(line, c).start()

    def start_side(line, dx):
        for c in range(CUTS):
            @pl.when(by_side(line, c))
            def _():
                side_copy(line, dx, line, at(z, dx), c).start()

            @pl.when(among(line, COLUMN[c]))
            def _():
                side_copy(line, dx, z, at(line, 0), c).start()

    def back_copy(block):
        return pltpu.make_async_remote_copy(
            src_ref=back_out.at[block], dst_ref=back_in.at[me],
            send_sem=back_send.at[block], recv_sem=back_recv.at[me],
            device_id={"expert": block}, device_id_type=MESH,
        )

    for half in range(2):
        loads[half].wait()
        forward(z, half)
    for d in range(1, blocks):
        route_copy(d).start()
    for copy in weights:
        copy.wait()

    last_dims = (((1,), (1,)), ((), ()))
    first = me * local
    diagonal = lax.broadcasted_iota(jnp.int32, (tok, tok), 0) == lax.broadcasted_iota(
        jnp.int32, (tok, tok), 1
    )
    back_row = lax.broadcasted_iota(jnp.int32, back_out.shape[1:], 0)

    def compute(block):
        pre = jnp.dot(acts[block], w_in[...], preferred_element_type=jnp.float32)
        back_all = lax.dot_general(
            grads[block], w_down[...], last_dims, preferred_element_type=jnp.float32
        )
        block_routes = routes[block]
        route_rows = jnp.zeros(back_out.shape[1:], jnp.float32)
        for e in range(local):
            route = jnp.sum(jnp.where(expert_row == first + e, block_routes, 0.0), axis=0, keepdims=True)
            route = jnp.sum(jnp.where(diagonal, route, 0.0), axis=1, keepdims=True)
            gate = pre[:, 2 * e * hidden : (2 * e + 1) * hidden]
            up = pre[:, (2 * e + 1) * hidden : (2 * e + 2) * hidden]
            back = back_all[:, e * hidden : (e + 1) * hidden]
            sig = jax.nn.sigmoid(gate)
            silu = gate * sig
            active = silu * up
            route_grad = jnp.sum(active * back, axis=1, keepdims=True)
            route_grad = jnp.sum(jnp.where(diagonal, route_grad, 0.0), axis=0, keepdims=True)
            route_rows = route_rows + jnp.where(back_row == e, route_grad, 0.0)
            back = back * route
            hidden_grads[block, :, pl.ds(2 * e * hidden, hidden)] = (
                back * up * sig * (1.0 + gate * (1.0 - sig))
            ).astype(jnp.bfloat16)
            hidden_grads[block, :, pl.ds((2 * e + 1) * hidden, hidden)] = (back * silu).astype(jnp.bfloat16)
            scaled_all[block, :, pl.ds(e * hidden, hidden)] = (active * route).astype(jnp.bfloat16)
        total = lax.dot_general(
            hidden_grads[block], w_in[...], last_dims, preferred_element_type=jnp.float32
        )
        back_out[block] = route_rows
        return total.astype(jnp.bfloat16)

    def step(j, carry):
        after_first = j - 1
        group = jnp.where(j == 0, 0, after_first // rows + 1)
        dx = jnp.where(j == 0, 0, lax.rem(after_first + rows, rows) + jnp.where(group == lines, 1, 0))
        line = line_at(group - jnp.where(dx > 0, 1, 0))
        block = at(line, dx)

        @pl.when((dx == 0) & (j > 0))
        def _():
            for half in range(2):
                arrived(block, half)
                forward(line, half)

        last_forward = (lines - 2) * rows + 1

        @pl.when(j == last_forward)
        def _():
            for k in range(lines - 1):
                start_col(line_at(k))
            for k in range(1, lines - 2):
                for other in range(1, rows):
                    start_side(line_at(k), other)

        @pl.when(dx > 0)
        def _():
            for half in range(2):
                arrived(block, half)

        @pl.when(j > 0)
        def _():
            pltpu.make_async_remote_copy(
                src_ref=routes.at[block], dst_ref=routes.at[block],
                send_sem=route_send.at[0], recv_sem=route_recv.at[block],
                device_id={"expert": at(z, 1)}, device_id_type=MESH,
            ).wait_recv()

        total = compute(block)

        @pl.when(j > 0)
        def _():
            back_copy(block).start()

        @pl.when(dx == 0)
        def _():
            col_out[line] = total

            @pl.when(j >= last_forward)
            def _():
                start_col(line)

        @pl.when(dx > 0)
        def _():
            side_out[line, dx - 1] = total

            @pl.when(j >= last_forward)
            def _():
                start_side(line, dx)

        return carry

    lax.fori_loop(0, blocks, step, 0)

    def side_arrived(line, dx, c):
        side_copy(line, dx, line, at(z, 1), c).wait_recv()

    for c in range(CUTS):
        for k in range(1, lines):
            line = line_at(k)

            @pl.when(by_side(line, c))
            def _():
                value = col_out[line, cuts[c]].astype(jnp.float32)
                for dx in range(1, rows):
                    side_arrived(line, dx, c)
                    value = value + side_in[line, dx - 1, cuts[c]].astype(jnp.float32)
                col_out[line, cuts[c]] = value.astype(jnp.bfloat16)
                col_copy(line, c).start()

        for dx in range(1, rows):
            for line in range(lines):
                @pl.when(among(line, COLUMN[c]))
                def _():
                    side_arrived(line, dx, c)
                    side_out[z, dx - 1, cuts[c]] = (
                        side_out[z, dx - 1, cuts[c]].astype(jnp.float32)
                        + side_in[line, dx - 1, cuts[c]].astype(jnp.float32)
                    ).astype(jnp.bfloat16)
            side_copy(z, dx, z, at(z, dx), c, before).start()

    first_dims = (((0,), (0,)), ((), ()))
    all_rows = blocks * tok
    tile = 256 if width % 256 == 0 and (local * hidden) % 256 == 0 else 128

    @pl.loop(0, width // tile)
    def _(c):
        at_c = pl.ds(pl.multiple_of(c * tile, tile), tile)
        left = acts[:, :, at_c].reshape(all_rows, tile)
        right = hidden_grads[...].reshape(all_rows, 2 * local * hidden)
        update = lax.dot_general(
            left, right, first_dims, preferred_element_type=jnp.float32
        ).astype(jnp.bfloat16)
        for e in range(local):
            gate_ref[e, at_c, :] = update[:, 2 * e * hidden : (2 * e + 1) * hidden]
            up_out_ref[e, at_c, :] = update[:, (2 * e + 1) * hidden : (2 * e + 2) * hidden]

    down_tile = 128
    for e in range(local):
        @pl.loop(0, hidden // down_tile)
        def _(c):
            at_left = pl.ds(pl.multiple_of(e * hidden + c * down_tile, down_tile), down_tile)
            at_c = pl.ds(pl.multiple_of(c * down_tile, down_tile), down_tile)
            left = scaled_all[:, :, at_left].reshape(all_rows, down_tile)
            right = grads[...].reshape(all_rows, width)
            down_ref[e, at_c, :] = lax.dot_general(
                left, right, first_dims, preferred_element_type=jnp.float32
            ).astype(jnp.bfloat16)

    for c in range(CUTS):
        value = jnp.zeros((cut_rows, width), jnp.float32)
        for dx in range(1, rows):
            side_arrived(z, dx, c)
            value = value + side_in[z, dx - 1, cuts[c]].astype(jnp.float32)
        for dz in range(lines):
            line = lax.rem(z + dz, lines)
            pltpu.make_async_remote_copy(
                src_ref=col_out.at[line, cuts[c]], dst_ref=col_in.at[line, cuts[c]],
                send_sem=col_send.at[line, c], recv_sem=col_recv.at[line, c],
                device_id={"expert": at(line, 0), "section": before}, device_id_type=MESH,
            ).wait_recv()
            value = value + col_in[line, cuts[c]].astype(jnp.float32)
        up_ref[cuts[c], :] = jnp.where(section == sections - 1, 0.0, value).astype(jnp.bfloat16)

    back_in[me] = back_out[me]
    for d in range(1, blocks):
        other = lax.rem(me + d, blocks)
        pltpu.make_async_remote_copy(
            src_ref=back_out.at[other], dst_ref=back_in.at[other],
            send_sem=back_send.at[other], recv_sem=back_recv.at[other],
            device_id={"expert": other}, device_id_type=MESH,
        ).wait_recv()
    route_total = jnp.zeros(ids.shape, jnp.float32)
    for b in range(blocks):
        rows_of = back_in[b]
        for e in range(local):
            route_total = route_total + jnp.where(ids == b * local + e, rows_of[e : e + 1, :], 0.0)
    own_route_ref[...] = route_total.astype(jnp.bfloat16)

    for line in range(lines):
        for half in range(2):
            for side in (1, -1):
                @pl.when(passes(line, side))
                def _():
                    z_copy(line, side, half).wait_send()
            for dx in range(1, rows):
                x_copy(line, dx, half).wait_send()
    for d in range(1, blocks):
        other = lax.rem(me + d, blocks)
        route_copy(d).wait_send()
        back_copy(other).wait_send()
    for line in range(lines):
        for c in range(CUTS):
            col_copy(line, c).wait_send()

        for dx in range(1, rows):
            for c in range(CUTS):
                side_copy(line, dx, z, at(z, dx), c).wait_send()


def finish(*refs):
    sources, targets, sem = refs[:5], refs[5:10], refs[10]
    copies = [pltpu.make_async_copy(a, b, sem.at[i]) for i, (a, b) in enumerate(zip(sources, targets))]
    for copy in copies:
        copy.start()
    for copy in copies:
        copy.wait()


def body(rows, inputs, out_grads, expert_ids, route_levels, w_gate, w_up, w_down):
    tok, width = inputs.shape[1:]
    local, _, hidden = w_gate.shape[1:]
    blocks = lax.axis_size("expert")
    sections = lax.axis_size("section")
    lines = blocks // rows
    experts = blocks * local
    top = expert_ids.shape[2]
    bf16 = jnp.bfloat16
    f32 = jnp.float32
    anywhere = pl.BlockSpec(memory_space=pl.ANY)
    inside = pl.BlockSpec(memory_space=pltpu.VMEM)
    dma = pltpu.SemaphoreType.DMA
    side = max(rows - 1, 1)
    back_rows = -(-local // 8) * 8
    shapes = ((tok, width), (top, tok), w_gate.shape[1:], w_up.shape[1:], w_down.shape[1:])
    limit = 66_900_000 - 2 * sum(-(-math.prod(shape) // 4096) * 4096 for shape in shapes)
    results = pl.pallas_call(
        functools.partial(kernel, lines, rows, sections),
        out_shape=tuple(pltpu.VMEM(shape, bf16) for shape in shapes),
        in_specs=[anywhere] * 7,
        out_specs=(inside,) * 5,
        scratch_shapes=[
            pltpu.VMEM((blocks, tok, width), bf16),
            pltpu.VMEM((blocks, tok, width), bf16),
            pltpu.VMEM((blocks, experts, tok), f32),
            pltpu.VMEM((width, 2 * local * hidden), bf16),
            pltpu.VMEM((local * hidden, width), bf16),
            pltpu.VMEM((blocks, tok, 2 * local * hidden), bf16),
            pltpu.VMEM((blocks, tok, local * hidden), bf16),
            pltpu.VMEM((lines, tok, width), bf16),
            pltpu.VMEM((lines, tok, width), bf16),
            pltpu.VMEM((lines, side, tok, width), bf16),
            pltpu.VMEM((lines, side, tok, width), bf16),
            pltpu.VMEM((blocks, back_rows, tok), f32),
            pltpu.VMEM((blocks, back_rows, tok), f32),
            pltpu.VMEM((top, tok), jnp.int32),
            pltpu.VMEM((top, tok), jnp.int32),
            dma((2,)),
            dma((2,)),
            dma((3 * local,)),
            dma((lines, 2, 2)),
            dma((lines, rows, 2)),
            dma((blocks,)),
            dma((blocks,)),
            dma((blocks,)),
            dma((blocks,)),
            dma((lines, CUTS)),
            dma((lines, CUTS)),
            dma((lines, side, CUTS)),
            dma((lines, side, CUTS)),
            dma((blocks,)),
            dma((blocks,)),
        ],
        compiler_params=pltpu.CompilerParams(
            collective_id=0, has_side_effects=True, vmem_limit_bytes=limit
        ),
    )(
        jnp.swapaxes(expert_ids[0], 0, 1), jnp.swapaxes(route_levels[0], 0, 1),
        inputs[0], out_grads[0], w_gate[0], w_up[0], w_down[0],
    )
    upstream, own_routes, gates, ups, downs = pl.pallas_call(
        finish,
        out_shape=tuple(jax.ShapeDtypeStruct(shape, bf16) for shape in shapes),
        in_specs=[inside] * 5,
        out_specs=(anywhere,) * 5,
        scratch_shapes=[dma((5,))],
        compiler_params=pltpu.CompilerParams(vmem_limit_bytes=1_000_000),
    )(*[pltpu.with_memory_space_constraint(r, pltpu.VMEM) for r in results])
    token_route = jnp.swapaxes(own_routes, 0, 1)
    return (upstream[None], token_route[None], gates[None], ups[None], downs[None])


def solution(mesh):
    blocks = mesh.shape["expert"]
    rows = math.isqrt(max(blocks // 2, 1))
    while blocks % rows:
        rows -= 1
    in_specs = (
        P("section", "expert", None),
        P("section", "expert", None),
        P("section", "expert", None),
        P("section", "expert", None),
        P("section", "expert", None, None),
        P("section", "expert", None, None),
        P("section", "expert", None, None),
    )
    out_specs = (
        P("section", "expert", None),
        P("section", "expert", None),
        P("section", "expert", None, None),
        P("section", "expert", None, None),
        P("section", "expert", None, None),
    )
    return jax.shard_map(
        functools.partial(body, rows), mesh=mesh, in_specs=in_specs, out_specs=out_specs, check_vma=False
    )
```

```python
import functools
import math

import jax
import jax.numpy as jnp
from jax import lax
from jax.experimental import pallas as pl
from jax.experimental.pallas import tpu as pltpu
from jax.sharding import PartitionSpec as P

MESH = pl.DeviceIdType.MESH
COLUMN = ((1,), (1,))
CUTS = len(COLUMN)


def kernel(
    lines, rows, sections,
    ids_ref, levels_ref, in_ref, grad_ref, wg_ref, wu_ref, wd_ref,
    up_ref, own_route_ref, gate_ref, up_out_ref, down_ref,
    acts, grads, routes, w_in, w_down, hidden_grads, scaled_all,
    col_out, col_in, side_out, side_in, back_out, back_in, ids_in, levels_in,
    small_sem, load_sem, weight_sem,
    z_send, x_send, act_recv, grad_recv, route_send, route_recv,
    col_send, col_recv, side_send, side_recv, back_send, back_recv,
):
    blocks = lines * rows
    tok, width = in_ref.shape
    local, _, hidden = wg_ref.shape
    experts = blocks * local
    me = lax.axis_index("expert")
    section = lax.axis_index("section")
    z, x = me // rows, lax.rem(me, rows)

    def at(line, dx):
        return line * rows + lax.rem(x + dx, rows)

    nearest_end = jnp.minimum(z, lines - 1 - z)
    inward = jnp.where(2 * z < lines, 1, -1)

    def line_at(k):
        both = k <= 2 * nearest_end
        far = jnp.where(both, (k + 1) // 2, k - nearest_end)
        sign = jnp.where(both & (lax.rem(k, 2) == 0), -inward, inward)
        return z + far * sign

    small = [
        pltpu.make_async_copy(ids_ref, ids_in, small_sem.at[0]),
        pltpu.make_async_copy(levels_ref, levels_in, small_sem.at[1]),
    ]
    for copy in small:
        copy.start()
    loads = [
        pltpu.make_async_copy(in_ref, acts.at[me], load_sem.at[0]),
        pltpu.make_async_copy(grad_ref, grads.at[me], load_sem.at[1]),
    ]
    weights = []
    for e in range(local):
        weights.append((wg_ref.at[e], w_in.at[:, pl.ds(2 * e * hidden, hidden)]))
        weights.append((wu_ref.at[e], w_in.at[:, pl.ds((2 * e + 1) * hidden, hidden)]))
        weights.append((wd_ref.at[e], w_down.at[pl.ds(e * hidden, hidden), :]))
    weights = [pltpu.make_async_copy(a, b, weight_sem.at[i]) for i, (a, b) in enumerate(weights)]
    for copy in loads + weights:
        copy.start()

    barrier = pltpu.get_barrier_semaphore()
    for d in range(1, blocks):
        pl.semaphore_signal(
            barrier, inc=1, device_id={"expert": lax.rem(me + d, blocks)}, device_id_type=MESH
        )
    before = lax.rem(section + sections - 1, sections)
    after = lax.rem(section + 1, sections)
    for dz in range(lines):
        line = lax.rem(z + dz, lines)
        for dx in range(rows if dz == 0 else 1):
            pl.semaphore_signal(
                barrier, inc=1, device_id={"expert": at(line, dx), "section": after}, device_id_type=MESH
            )

    for copy in small:
        copy.wait()
    ids = ids_in[...]
    levels = levels_in[...]
    expert_row = lax.broadcasted_iota(jnp.int32, (experts, tok), 0)
    mine_routes = jnp.zeros((experts, tok), jnp.float32)
    for k in range(ids.shape[0]):
        level = levels[k : k + 1, :].astype(jnp.float32) * (1.0 / 256.0)
        mine_routes = mine_routes + jnp.where(ids[k : k + 1, :] == expert_row, level, 0.0)
    routes[me] = mine_routes

    pl.semaphore_wait(barrier, blocks - 1 + lines + rows - 1)

    halves = ((acts, act_recv), (grads, grad_recv))

    def z_copy(line, side, half):
        buffer, recv = halves[half]
        block = at(line, 0)
        return pltpu.make_async_remote_copy(
            src_ref=buffer.at[block], dst_ref=buffer.at[block],
            send_sem=z_send.at[line, (side + 1) // 2, half], recv_sem=recv.at[block],
            device_id={"expert": me + side * rows}, device_id_type=MESH,
        )

    def x_copy(line, dx, half):
        buffer, recv = halves[half]
        block = at(line, 0)
        return pltpu.make_async_remote_copy(
            src_ref=buffer.at[block], dst_ref=buffer.at[block],
            send_sem=x_send.at[line, dx, half], recv_sem=recv.at[block],
            device_id={"expert": at(z, dx)}, device_id_type=MESH,
        )

    def arrived(block, half):
        buffer, recv = halves[half]
        pltpu.make_async_remote_copy(
            src_ref=buffer.at[block], dst_ref=buffer.at[block],
            send_sem=x_send.at[0, 0, half], recv_sem=recv.at[block],
            device_id={"expert": at(z, 1)}, device_id_type=MESH,
        ).wait_recv()

    def passes(line, side):
        if side > 0:
            return (line <= z) & (z < lines - 1)
        return (line >= z) & (z > 0)

    def forward(line, half):
        for side in (1, -1):
            @pl.when(passes(line, side))
            def _():
                z_copy(line, side, half).start()
        for dx in range(1, rows):
            x_copy(line, dx, half).start()

    def route_copy(d):
        other = lax.rem(me + d, blocks)
        return pltpu.make_async_remote_copy(
            src_ref=routes.at[me], dst_ref=routes.at[me],
            send_sem=route_send.at[d], recv_sem=route_recv.at[me],
            device_id={"expert": other}, device_id_type=MESH,
        )

    def away(line):
        return jnp.abs(line - z)

    def among(line, distances):
        return functools.reduce(jnp.logical_or, [away(line) == d for d in distances], line != line)

    def by_side(line, c):
        return (line != z) & ~among(line, COLUMN[c])

    cut_rows = tok // CUTS
    cuts = [pl.ds(c * cut_rows, cut_rows) for c in range(CUTS)]

    def col_copy(line, c):
        return pltpu.make_async_remote_copy(
            src_ref=col_out.at[line, cuts[c]], dst_ref=col_in.at[z, cuts[c]],
            send_sem=col_send.at[line, c], recv_sem=col_recv.at[z, c],
            device_id={"expert": at(line, 0), "section": before}, device_id_type=MESH,
        )

    def side_copy(line, dx, slot, target, c, home=None):
        return pltpu.make_async_remote_copy(
            src_ref=side_out.at[line, dx - 1, cuts[c]], dst_ref=side_in.at[slot, dx - 1, cuts[c]],
            send_sem=side_send.at[line, dx - 1, c], recv_sem=side_recv.at[slot, dx - 1, c],
            device_id={"expert": target, "section": section if home is None else home},
            device_id_type=MESH,
        )

    def start_col(line):
        for c in range(CUTS):
            @pl.when(~by_side(line, c))
            def _():
                col_copy(line, c).start()

    def start_side(line, dx):
        for c in range(CUTS):
            @pl.when(by_side(line, c))
            def _():
                side_copy(line, dx, line, at(z, dx), c).start()

            @pl.when(among(line, COLUMN[c]))
            def _():
                side_copy(line, dx, z, at(line, 0), c).start()

    def back_copy(block):
        return pltpu.make_async_remote_copy(
            src_ref=back_out.at[block], dst_ref=back_in.at[me],
            send_sem=back_send.at[block], recv_sem=back_recv.at[me],
            device_id={"expert": block}, device_id_type=MESH,
        )

    for half in range(2):
        loads[half].wait()
        forward(z, half)
    for d in range(1, blocks):
        route_copy(d).start()
    for copy in weights:
        copy.wait()

    last_dims = (((1,), (1,)), ((), ()))
    first = me * local
    diagonal = lax.broadcasted_iota(jnp.int32, (tok, tok), 0) == lax.broadcasted_iota(
        jnp.int32, (tok, tok), 1
    )
    back_row = lax.broadcasted_iota(jnp.int32, back_out.shape[1:], 0)

    def compute(block, wait_grads):
        pre = jnp.dot(acts[block], w_in[...], preferred_element_type=jnp.float32)
        forward_parts = []
        for e in range(local):
            gate = pre[:, 2 * e * hidden : (2 * e + 1) * hidden]
            up = pre[:, (2 * e + 1) * hidden : (2 * e + 2) * hidden]
            sig = jax.nn.sigmoid(gate)
            silu = gate * sig
            forward_parts.append((silu, silu * up, up * sig * (1.0 + gate * (1.0 - sig))))
        wait_grads()
        back_all = lax.dot_general(
            grads[block], w_down[...], last_dims, preferred_element_type=jnp.float32
        )
        block_routes = routes[block]
        route_rows = jnp.zeros(back_out.shape[1:], jnp.float32)
        for e in range(local):
            route = jnp.sum(jnp.where(expert_row == first + e, block_routes, 0.0), axis=0, keepdims=True)
            route = jnp.sum(jnp.where(diagonal, route, 0.0), axis=1, keepdims=True)
            silu, active, slope = forward_parts[e]
            back = back_all[:, e * hidden : (e + 1) * hidden]
            route_grad = jnp.sum(active * back, axis=1, keepdims=True)
            route_grad = jnp.sum(jnp.where(diagonal, route_grad, 0.0), axis=0, keepdims=True)
            route_rows = route_rows + jnp.where(back_row == e, route_grad, 0.0)
            back = back * route
            hidden_grads[block, :, pl.ds(2 * e * hidden, hidden)] = (
                back * slope
            ).astype(jnp.bfloat16)
            hidden_grads[block, :, pl.ds((2 * e + 1) * hidden, hidden)] = (back * silu).astype(jnp.bfloat16)
            scaled_all[block, :, pl.ds(e * hidden, hidden)] = (active * route).astype(jnp.bfloat16)
        total = lax.dot_general(
            hidden_grads[block], w_in[...], last_dims, preferred_element_type=jnp.float32
        )
        back_out[block] = route_rows
        return total.astype(jnp.bfloat16)

    def step(j, carry):
        after_first = j - 1
        group = jnp.where(j == 0, 0, after_first // rows + 1)
        dx = jnp.where(j == 0, 0, lax.rem(after_first + rows, rows) + jnp.where(group == lines, 1, 0))
        line = line_at(group - jnp.where(dx > 0, 1, 0))
        block = at(line, dx)

        def receive(half):
            @pl.when(j > 0)
            def _():
                arrived(block, half)

            @pl.when((dx == 0) & (j > 0))
            def _():
                forward(line, half)

        receive(0)

        last_forward = (lines - 2) * rows + 1

        def wait_grads():
            receive(1)

            @pl.when(j == last_forward)
            def _():
                for k in range(lines - 1):
                    start_col(line_at(k))
                for k in range(1, lines - 2):
                    for other in range(1, rows):
                        start_side(line_at(k), other)

        @pl.when(j > 0)
        def _():
            pltpu.make_async_remote_copy(
                src_ref=routes.at[block], dst_ref=routes.at[block],
                send_sem=route_send.at[0], recv_sem=route_recv.at[block],
                device_id={"expert": at(z, 1)}, device_id_type=MESH,
            ).wait_recv()

        total = compute(block, wait_grads)

        @pl.when(j > 0)
        def _():
            back_copy(block).start()

        @pl.when(dx == 0)
        def _():
            col_out[line] = total

            @pl.when(j >= last_forward)
            def _():
                start_col(line)

        @pl.when(dx > 0)
        def _():
            side_out[line, dx - 1] = total

            @pl.when(j >= last_forward)
            def _():
                start_side(line, dx)

        return carry

    lax.fori_loop(0, blocks, step, 0)

    def side_arrived(line, dx, c):
        side_copy(line, dx, line, at(z, 1), c).wait_recv()

    for c in range(CUTS):
        for k in range(1, lines):
            line = line_at(k)

            @pl.when(by_side(line, c))
            def _():
                value = col_out[line, cuts[c]].astype(jnp.float32)
                for dx in range(1, rows):
                    side_arrived(line, dx, c)
                    value = value + side_in[line, dx - 1, cuts[c]].astype(jnp.float32)
                col_out[line, cuts[c]] = value.astype(jnp.bfloat16)
                col_copy(line, c).start()

        for dx in range(1, rows):
            for line in range(lines):
                @pl.when(among(line, COLUMN[c]))
                def _():
                    side_arrived(line, dx, c)
                    side_out[z, dx - 1, cuts[c]] = (
                        side_out[z, dx - 1, cuts[c]].astype(jnp.float32)
                        + side_in[line, dx - 1, cuts[c]].astype(jnp.float32)
                    ).astype(jnp.bfloat16)
            side_copy(z, dx, z, at(z, dx), c, before).start()

    first_dims = (((0,), (0,)), ((), ()))
    all_rows = blocks * tok
    tile = 256 if width % 256 == 0 and (local * hidden) % 256 == 0 else 128

    @pl.loop(0, width // tile)
    def _(c):
        at_c = pl.ds(pl.multiple_of(c * tile, tile), tile)
        left = acts[:, :, at_c].reshape(all_rows, tile)
        right = hidden_grads[...].reshape(all_rows, 2 * local * hidden)
        update = lax.dot_general(
            left, right, first_dims, preferred_element_type=jnp.float32
        ).astype(jnp.bfloat16)
        for e in range(local):
            gate_ref[e, at_c, :] = update[:, 2 * e * hidden : (2 * e + 1) * hidden]
            up_out_ref[e, at_c, :] = update[:, (2 * e + 1) * hidden : (2 * e + 2) * hidden]

    down_tile = 128
    for e in range(local):
        @pl.loop(0, hidden // down_tile)
        def _(c):
            at_left = pl.ds(pl.multiple_of(e * hidden + c * down_tile, down_tile), down_tile)
            at_c = pl.ds(pl.multiple_of(c * down_tile, down_tile), down_tile)
            left = scaled_all[:, :, at_left].reshape(all_rows, down_tile)
            right = grads[...].reshape(all_rows, width)
            down_ref[e, at_c, :] = lax.dot_general(
                left, right, first_dims, preferred_element_type=jnp.float32
            ).astype(jnp.bfloat16)

    back_in[me] = back_out[me]
    for d in range(1, blocks):
        other = lax.rem(me + d, blocks)
        pltpu.make_async_remote_copy(
            src_ref=back_out.at[other], dst_ref=back_in.at[other],
            send_sem=back_send.at[other], recv_sem=back_recv.at[other],
            device_id={"expert": other}, device_id_type=MESH,
        ).wait_recv()
    route_total = jnp.zeros(ids.shape, jnp.float32)
    for b in range(blocks):
        rows_of = back_in[b]
        for e in range(local):
            route_total = route_total + jnp.where(ids == b * local + e, rows_of[e : e + 1, :], 0.0)
    own_route_ref[...] = route_total.astype(jnp.bfloat16)

    for c in range(CUTS):
        value = jnp.zeros((cut_rows, width), jnp.float32)
        for dx in range(1, rows):
            side_arrived(z, dx, c)
            value = value + side_in[z, dx - 1, cuts[c]].astype(jnp.float32)
        for dz in range(lines):
            line = lax.rem(z + dz, lines)
            pltpu.make_async_remote_copy(
                src_ref=col_out.at[line, cuts[c]], dst_ref=col_in.at[line, cuts[c]],
                send_sem=col_send.at[line, c], recv_sem=col_recv.at[line, c],
                device_id={"expert": at(line, 0), "section": before}, device_id_type=MESH,
            ).wait_recv()
            value = value + col_in[line, cuts[c]].astype(jnp.float32)
        up_ref[cuts[c], :] = jnp.where(section == sections - 1, 0.0, value).astype(jnp.bfloat16)

    for line in range(lines):
        for half in range(2):
            for side in (1, -1):
                @pl.when(passes(line, side))
                def _():
                    z_copy(line, side, half).wait_send()
            for dx in range(1, rows):
                x_copy(line, dx, half).wait_send()
    for d in range(1, blocks):
        other = lax.rem(me + d, blocks)
        route_copy(d).wait_send()
        back_copy(other).wait_send()
    for line in range(lines):
        for c in range(CUTS):
            col_copy(line, c).wait_send()

        for dx in range(1, rows):
            for c in range(CUTS):
                side_copy(line, dx, z, at(z, dx), c).wait_send()


def finish(*refs):
    sources, targets, sem = refs[:5], refs[5:10], refs[10]
    copies = [pltpu.make_async_copy(a, b, sem.at[i]) for i, (a, b) in enumerate(zip(sources, targets))]
    for copy in copies:
        copy.start()
    for copy in copies:
        copy.wait()


def body(rows, inputs, out_grads, expert_ids, route_levels, w_gate, w_up, w_down):
    tok, width = inputs.shape[1:]
    local, _, hidden = w_gate.shape[1:]
    blocks = lax.axis_size("expert")
    sections = lax.axis_size("section")
    lines = blocks // rows
    experts = blocks * local
    top = expert_ids.shape[2]
    bf16 = jnp.bfloat16
    f32 = jnp.float32
    anywhere = pl.BlockSpec(memory_space=pl.ANY)
    inside = pl.BlockSpec(memory_space=pltpu.VMEM)
    dma = pltpu.SemaphoreType.DMA
    side = max(rows - 1, 1)
    back_rows = -(-local // 8) * 8
    shapes = ((tok, width), (top, tok), w_gate.shape[1:], w_up.shape[1:], w_down.shape[1:])
    limit = 66_900_000 - 2 * sum(-(-math.prod(shape) // 4096) * 4096 for shape in shapes)
    results = pl.pallas_call(
        functools.partial(kernel, lines, rows, sections),
        out_shape=tuple(pltpu.VMEM(shape, bf16) for shape in shapes),
        in_specs=[anywhere] * 7,
        out_specs=(inside,) * 5,
        scratch_shapes=[
            pltpu.VMEM((blocks, tok, width), bf16),
            pltpu.VMEM((blocks, tok, width), bf16),
            pltpu.VMEM((blocks, experts, tok), f32),
            pltpu.VMEM((width, 2 * local * hidden), bf16),
            pltpu.VMEM((local * hidden, width), bf16),
            pltpu.VMEM((blocks, tok, 2 * local * hidden), bf16),
            pltpu.VMEM((blocks, tok, local * hidden), bf16),
            pltpu.VMEM((lines, tok, width), bf16),
            pltpu.VMEM((lines, tok, width), bf16),
            pltpu.VMEM((lines, side, tok, width), bf16),
            pltpu.VMEM((lines, side, tok, width), bf16),
            pltpu.VMEM((blocks, back_rows, tok), f32),
            pltpu.VMEM((blocks, back_rows, tok), f32),
            pltpu.VMEM((top, tok), jnp.int32),
            pltpu.VMEM((top, tok), jnp.int32),
            dma((2,)),
            dma((2,)),
            dma((3 * local,)),
            dma((lines, 2, 2)),
            dma((lines, rows, 2)),
            dma((blocks,)),
            dma((blocks,)),
            dma((blocks,)),
            dma((blocks,)),
            dma((lines, CUTS)),
            dma((lines, CUTS)),
            dma((lines, side, CUTS)),
            dma((lines, side, CUTS)),
            dma((blocks,)),
            dma((blocks,)),
        ],
        compiler_params=pltpu.CompilerParams(
            collective_id=0, has_side_effects=True, vmem_limit_bytes=limit
        ),
    )(
        jnp.swapaxes(expert_ids[0], 0, 1), jnp.swapaxes(route_levels[0], 0, 1),
        inputs[0], out_grads[0], w_gate[0], w_up[0], w_down[0],
    )
    upstream, own_routes, gates, ups, downs = pl.pallas_call(
        finish,
        out_shape=tuple(jax.ShapeDtypeStruct(shape, bf16) for shape in shapes),
        in_specs=[inside] * 5,
        out_specs=(anywhere,) * 5,
        scratch_shapes=[dma((5,))],
        compiler_params=pltpu.CompilerParams(vmem_limit_bytes=1_000_000),
    )(*[pltpu.with_memory_space_constraint(r, pltpu.VMEM) for r in results])
    token_route = jnp.swapaxes(own_routes, 0, 1)
    return (upstream[None], token_route[None], gates[None], ups[None], downs[None])


def solution(mesh):
    blocks = mesh.shape["expert"]
    rows = math.isqrt(max(blocks // 2, 1))
    while blocks % rows:
        rows -= 1
    in_specs = (
        P("section", "expert", None),
        P("section", "expert", None),
        P("section", "expert", None),
        P("section", "expert", None),
        P("section", "expert", None, None),
        P("section", "expert", None, None),
        P("section", "expert", None, None),
    )
    out_specs = (
        P("section", "expert", None),
        P("section", "expert", None),
        P("section", "expert", None, None),
        P("section", "expert", None, None),
        P("section", "expert", None, None),
    )
    return jax.shard_map(
        functools.partial(body, rows), mesh=mesh, in_specs=in_specs, out_specs=out_specs, check_vma=False
    )
```

```python
import functools
import math

import jax
import jax.numpy as jnp
from jax import lax
from jax.experimental import pallas as pl
from jax.experimental.pallas import tpu as pltpu
from jax.sharding import PartitionSpec as P

MESH = pl.DeviceIdType.MESH
COLUMN = ((1,), (1,), (1,), (1,))
CUTS = len(COLUMN)


def kernel(
    lines, rows, sections,
    ids_ref, levels_ref, in_ref, grad_ref, wg_ref, wu_ref, wd_ref,
    up_ref, own_route_ref, gate_ref, up_out_ref, down_ref,
    acts, grads, routes, w_in, w_down, hidden_grads, scaled_all,
    col_out, col_in, side_out, side_in, back_out, back_in, ids_in, levels_in,
    small_sem, load_sem, weight_sem,
    z_send, x_send, act_recv, grad_recv, route_send, route_recv,
    col_send, col_recv, side_send, side_recv, back_send, back_recv,
):
    blocks = lines * rows
    tok, width = in_ref.shape
    local, _, hidden = wg_ref.shape
    experts = blocks * local
    me = lax.axis_index("expert")
    section = lax.axis_index("section")
    z, x = me // rows, lax.rem(me, rows)

    def at(line, dx):
        return line * rows + lax.rem(x + dx, rows)

    nearest_end = jnp.minimum(z, lines - 1 - z)
    inward = jnp.where(2 * z < lines, 1, -1)

    def line_at(k):
        both = k <= 2 * nearest_end
        far = jnp.where(both, (k + 1) // 2, k - nearest_end)
        sign = jnp.where(both & (lax.rem(k, 2) == 0), -inward, inward)
        return z + far * sign

    small = [
        pltpu.make_async_copy(ids_ref, ids_in, small_sem.at[0]),
        pltpu.make_async_copy(levels_ref, levels_in, small_sem.at[1]),
    ]
    for copy in small:
        copy.start()
    loads = [
        pltpu.make_async_copy(in_ref, acts.at[me], load_sem.at[0]),
        pltpu.make_async_copy(grad_ref, grads.at[me], load_sem.at[1]),
    ]
    weights = []
    for e in range(local):
        weights.append((wg_ref.at[e], w_in.at[:, pl.ds(2 * e * hidden, hidden)]))
        weights.append((wu_ref.at[e], w_in.at[:, pl.ds((2 * e + 1) * hidden, hidden)]))
        weights.append((wd_ref.at[e], w_down.at[pl.ds(e * hidden, hidden), :]))
    weights = [pltpu.make_async_copy(a, b, weight_sem.at[i]) for i, (a, b) in enumerate(weights)]
    for copy in loads + weights:
        copy.start()

    barrier = pltpu.get_barrier_semaphore()
    for d in range(1, blocks):
        pl.semaphore_signal(
            barrier, inc=1, device_id={"expert": lax.rem(me + d, blocks)}, device_id_type=MESH
        )
    before = lax.rem(section + sections - 1, sections)
    after = lax.rem(section + 1, sections)
    for dz in range(lines):
        line = lax.rem(z + dz, lines)
        for dx in range(rows if dz == 0 else 1):
            pl.semaphore_signal(
                barrier, inc=1, device_id={"expert": at(line, dx), "section": after}, device_id_type=MESH
            )

    for copy in small:
        copy.wait()
    ids = ids_in[...]
    levels = levels_in[...]
    expert_row = lax.broadcasted_iota(jnp.int32, (experts, tok), 0)
    mine_routes = jnp.zeros((experts, tok), jnp.float32)
    for k in range(ids.shape[0]):
        level = levels[k : k + 1, :].astype(jnp.float32) * (1.0 / 256.0)
        mine_routes = mine_routes + jnp.where(ids[k : k + 1, :] == expert_row, level, 0.0)
    routes[me] = mine_routes

    pl.semaphore_wait(barrier, blocks - 1 + lines + rows - 1)

    halves = ((acts, act_recv), (grads, grad_recv))

    def z_copy(line, side, half):
        buffer, recv = halves[half]
        block = at(line, 0)
        return pltpu.make_async_remote_copy(
            src_ref=buffer.at[block], dst_ref=buffer.at[block],
            send_sem=z_send.at[line, (side + 1) // 2, half], recv_sem=recv.at[block],
            device_id={"expert": me + side * rows}, device_id_type=MESH,
        )

    def x_copy(line, dx, half):
        buffer, recv = halves[half]
        block = at(line, 0)
        return pltpu.make_async_remote_copy(
            src_ref=buffer.at[block], dst_ref=buffer.at[block],
            send_sem=x_send.at[line, dx, half], recv_sem=recv.at[block],
            device_id={"expert": at(z, dx)}, device_id_type=MESH,
        )

    def arrived(block, half):
        buffer, recv = halves[half]
        pltpu.make_async_remote_copy(
            src_ref=buffer.at[block], dst_ref=buffer.at[block],
            send_sem=x_send.at[0, 0, half], recv_sem=recv.at[block],
            device_id={"expert": at(z, 1)}, device_id_type=MESH,
        ).wait_recv()

    def passes(line, side):
        if side > 0:
            return (line <= z) & (z < lines - 1)
        return (line >= z) & (z > 0)

    def forward(line, half):
        for side in (1, -1):
            @pl.when(passes(line, side))
            def _():
                z_copy(line, side, half).start()
        for dx in range(1, rows):
            x_copy(line, dx, half).start()

    def route_copy(d):
        other = lax.rem(me + d, blocks)
        return pltpu.make_async_remote_copy(
            src_ref=routes.at[me], dst_ref=routes.at[me],
            send_sem=route_send.at[d], recv_sem=route_recv.at[me],
            device_id={"expert": other}, device_id_type=MESH,
        )

    def away(line):
        return jnp.abs(line - z)

    def among(line, distances):
        return functools.reduce(jnp.logical_or, [away(line) == d for d in distances], line != line)

    def by_side(line, c):
        return (line != z) & ~among(line, COLUMN[c])

    cut_rows = tok // CUTS
    cuts = [pl.ds(c * cut_rows, cut_rows) for c in range(CUTS)]

    def col_copy(line, c):
        return pltpu.make_async_remote_copy(
            src_ref=col_out.at[line, cuts[c]], dst_ref=col_in.at[z, cuts[c]],
            send_sem=col_send.at[line, c], recv_sem=col_recv.at[z, c],
            device_id={"expert": at(line, 0), "section": before}, device_id_type=MESH,
        )

    def side_copy(line, dx, slot, target, c, home=None):
        return pltpu.make_async_remote_copy(
            src_ref=side_out.at[line, dx - 1, cuts[c]], dst_ref=side_in.at[slot, dx - 1, cuts[c]],
            send_sem=side_send.at[line, dx - 1, c], recv_sem=side_recv.at[slot, dx - 1, c],
            device_id={"expert": target, "section": section if home is None else home},
            device_id_type=MESH,
        )

    def start_col(line):
        for c in range(CUTS):
            @pl.when(~by_side(line, c))
            def _():
                col_copy(line, c).start()

    def start_side(line, dx):
        for c in range(CUTS):
            @pl.when(by_side(line, c))
            def _():
                side_copy(line, dx, line, at(z, dx), c).start()

            @pl.when(among(line, COLUMN[c]))
            def _():
                side_copy(line, dx, z, at(line, 0), c).start()

    def back_copy(block):
        return pltpu.make_async_remote_copy(
            src_ref=back_out.at[block], dst_ref=back_in.at[me],
            send_sem=back_send.at[block], recv_sem=back_recv.at[me],
            device_id={"expert": block}, device_id_type=MESH,
        )

    for half in range(2):
        loads[half].wait()
        forward(z, half)
    for d in range(1, blocks):
        route_copy(d).start()
    for copy in weights:
        copy.wait()

    last_dims = (((1,), (1,)), ((), ()))
    first = me * local
    diagonal = lax.broadcasted_iota(jnp.int32, (tok, tok), 0) == lax.broadcasted_iota(
        jnp.int32, (tok, tok), 1
    )
    back_row = lax.broadcasted_iota(jnp.int32, back_out.shape[1:], 0)

    def compute(block, wait_grads):
        pre = jnp.dot(acts[block], w_in[...], preferred_element_type=jnp.float32)
        forward_parts = []
        for e in range(local):
            gate = pre[:, 2 * e * hidden : (2 * e + 1) * hidden]
            up = pre[:, (2 * e + 1) * hidden : (2 * e + 2) * hidden]
            sig = jax.nn.sigmoid(gate)
            silu = gate * sig
            forward_parts.append((silu, silu * up, up * sig * (1.0 + gate * (1.0 - sig))))
        wait_grads()
        back_all = lax.dot_general(
            grads[block], w_down[...], last_dims, preferred_element_type=jnp.float32
        )
        block_routes = routes[block]
        rest = []
        for e in range(local):
            route = jnp.sum(jnp.where(expert_row == first + e, block_routes, 0.0), axis=0, keepdims=True)
            route = jnp.sum(jnp.where(diagonal, route, 0.0), axis=1, keepdims=True)
            silu, active, slope = forward_parts[e]
            back = back_all[:, e * hidden : (e + 1) * hidden]
            rest.append((route, active, back))
            back = back * route
            hidden_grads[block, :, pl.ds(2 * e * hidden, hidden)] = (back * slope).astype(jnp.bfloat16)
            hidden_grads[block, :, pl.ds((2 * e + 1) * hidden, hidden)] = (back * silu).astype(jnp.bfloat16)
        total = lax.dot_general(
            hidden_grads[block], w_in[...], last_dims, preferred_element_type=jnp.float32
        )

        def finish_block():
            route_rows = jnp.zeros(back_out.shape[1:], jnp.float32)
            for e, (route, active, back) in enumerate(rest):
                route_grad = jnp.sum(active * back, axis=1, keepdims=True)
                route_grad = jnp.sum(jnp.where(diagonal, route_grad, 0.0), axis=0, keepdims=True)
                route_rows = route_rows + jnp.where(back_row == e, route_grad, 0.0)
                scaled_all[block, :, pl.ds(e * hidden, hidden)] = (active * route).astype(jnp.bfloat16)
            back_out[block] = route_rows

        return total.astype(jnp.bfloat16), finish_block

    def step(j, carry):
        after_first = j - 1
        group = jnp.where(j == 0, 0, after_first // rows + 1)
        dx = jnp.where(j == 0, 0, lax.rem(after_first + rows, rows) + jnp.where(group == lines, 1, 0))
        line = line_at(group - jnp.where(dx > 0, 1, 0))
        block = at(line, dx)

        def receive(half):
            @pl.when(j > 0)
            def _():
                arrived(block, half)

            @pl.when((dx == 0) & (j > 0))
            def _():
                forward(line, half)

        receive(0)

        last_forward = (lines - 2) * rows + 1

        def wait_grads():
            receive(1)

            @pl.when(j == last_forward)
            def _():
                for k in range(lines - 1):
                    start_col(line_at(k))
                for k in range(1, lines - 2):
                    for other in range(1, rows):
                        start_side(line_at(k), other)

        @pl.when(j > 0)
        def _():
            pltpu.make_async_remote_copy(
                src_ref=routes.at[block], dst_ref=routes.at[block],
                send_sem=route_send.at[0], recv_sem=route_recv.at[block],
                device_id={"expert": at(z, 1)}, device_id_type=MESH,
            ).wait_recv()

        total, finish_block = compute(block, wait_grads)

        @pl.when(dx == 0)
        def _():
            col_out[line] = total

            @pl.when(j >= last_forward)
            def _():
                start_col(line)

        @pl.when(dx > 0)
        def _():
            side_out[line, dx - 1] = total

            @pl.when(j >= last_forward)
            def _():
                start_side(line, dx)

        finish_block()

        @pl.when(j > 0)
        def _():
            back_copy(block).start()

        return carry

    lax.fori_loop(0, blocks, step, 0)

    def side_arrived(line, dx, c):
        side_copy(line, dx, line, at(z, 1), c).wait_recv()

    for c in range(CUTS):
        for k in range(1, lines):
            line = line_at(k)

            @pl.when(by_side(line, c))
            def _():
                value = col_out[line, cuts[c]].astype(jnp.float32)
                for dx in range(1, rows):
                    side_arrived(line, dx, c)
                    value = value + side_in[line, dx - 1, cuts[c]].astype(jnp.float32)
                col_out[line, cuts[c]] = value.astype(jnp.bfloat16)
                col_copy(line, c).start()

        for dx in range(1, rows):
            for line in range(lines):
                @pl.when(among(line, COLUMN[c]))
                def _():
                    side_arrived(line, dx, c)
                    side_out[z, dx - 1, cuts[c]] = (
                        side_out[z, dx - 1, cuts[c]].astype(jnp.float32)
                        + side_in[line, dx - 1, cuts[c]].astype(jnp.float32)
                    ).astype(jnp.bfloat16)
            side_copy(z, dx, z, at(z, dx), c, before).start()

    first_dims = (((0,), (0,)), ((), ()))
    all_rows = blocks * tok
    tile = 256 if width % 256 == 0 and (local * hidden) % 256 == 0 else 128

    @pl.loop(0, width // tile)
    def _(c):
        at_c = pl.ds(pl.multiple_of(c * tile, tile), tile)
        left = acts[:, :, at_c].reshape(all_rows, tile)
        right = hidden_grads[...].reshape(all_rows, 2 * local * hidden)
        update = lax.dot_general(
            left, right, first_dims, preferred_element_type=jnp.float32
        ).astype(jnp.bfloat16)
        for e in range(local):
            gate_ref[e, at_c, :] = update[:, 2 * e * hidden : (2 * e + 1) * hidden]
            up_out_ref[e, at_c, :] = update[:, (2 * e + 1) * hidden : (2 * e + 2) * hidden]

    down_tile = 128
    for e in range(local):
        @pl.loop(0, hidden // down_tile)
        def _(c):
            at_left = pl.ds(pl.multiple_of(e * hidden + c * down_tile, down_tile), down_tile)
            at_c = pl.ds(pl.multiple_of(c * down_tile, down_tile), down_tile)
            left = scaled_all[:, :, at_left].reshape(all_rows, down_tile)
            right = grads[...].reshape(all_rows, width)
            down_ref[e, at_c, :] = lax.dot_general(
                left, right, first_dims, preferred_element_type=jnp.float32
            ).astype(jnp.bfloat16)

    back_in[me] = back_out[me]
    for d in range(1, blocks):
        other = lax.rem(me + d, blocks)
        pltpu.make_async_remote_copy(
            src_ref=back_out.at[other], dst_ref=back_in.at[other],
            send_sem=back_send.at[other], recv_sem=back_recv.at[other],
            device_id={"expert": other}, device_id_type=MESH,
        ).wait_recv()
    route_total = jnp.zeros(ids.shape, jnp.float32)
    for b in range(blocks):
        rows_of = back_in[b]
        for e in range(local):
            route_total = route_total + jnp.where(ids == b * local + e, rows_of[e : e + 1, :], 0.0)
    own_route_ref[...] = route_total.astype(jnp.bfloat16)

    for c in range(CUTS):
        value = jnp.zeros((cut_rows, width), jnp.float32)
        for dx in range(1, rows):
            side_arrived(z, dx, c)
            value = value + side_in[z, dx - 1, cuts[c]].astype(jnp.float32)
        for dz in range(lines):
            line = lax.rem(z + dz, lines)
            pltpu.make_async_remote_copy(
                src_ref=col_out.at[line, cuts[c]], dst_ref=col_in.at[line, cuts[c]],
                send_sem=col_send.at[line, c], recv_sem=col_recv.at[line, c],
                device_id={"expert": at(line, 0), "section": before}, device_id_type=MESH,
            ).wait_recv()
            value = value + col_in[line, cuts[c]].astype(jnp.float32)
        up_ref[cuts[c], :] = jnp.where(section == sections - 1, 0.0, value).astype(jnp.bfloat16)

    for line in range(lines):
        for half in range(2):
            for side in (1, -1):
                @pl.when(passes(line, side))
                def _():
                    z_copy(line, side, half).wait_send()
            for dx in range(1, rows):
                x_copy(line, dx, half).wait_send()
    for d in range(1, blocks):
        other = lax.rem(me + d, blocks)
        route_copy(d).wait_send()
        back_copy(other).wait_send()
    for line in range(lines):
        for c in range(CUTS):
            col_copy(line, c).wait_send()

        for dx in range(1, rows):
            for c in range(CUTS):
                side_copy(line, dx, z, at(z, dx), c).wait_send()


def finish(*refs):
    sources, targets, sem = refs[:5], refs[5:10], refs[10]
    copies = [pltpu.make_async_copy(a, b, sem.at[i]) for i, (a, b) in enumerate(zip(sources, targets))]
    for copy in copies:
        copy.start()
    for copy in copies:
        copy.wait()


def body(rows, inputs, out_grads, expert_ids, route_levels, w_gate, w_up, w_down):
    tok, width = inputs.shape[1:]
    local, _, hidden = w_gate.shape[1:]
    blocks = lax.axis_size("expert")
    sections = lax.axis_size("section")
    lines = blocks // rows
    experts = blocks * local
    top = expert_ids.shape[2]
    bf16 = jnp.bfloat16
    f32 = jnp.float32
    anywhere = pl.BlockSpec(memory_space=pl.ANY)
    inside = pl.BlockSpec(memory_space=pltpu.VMEM)
    dma = pltpu.SemaphoreType.DMA
    side = max(rows - 1, 1)
    back_rows = -(-local // 8) * 8
    shapes = ((tok, width), (top, tok), w_gate.shape[1:], w_up.shape[1:], w_down.shape[1:])
    limit = 66_900_000 - 2 * sum(-(-math.prod(shape) // 4096) * 4096 for shape in shapes)
    results = pl.pallas_call(
        functools.partial(kernel, lines, rows, sections),
        out_shape=tuple(pltpu.VMEM(shape, bf16) for shape in shapes),
        in_specs=[anywhere] * 7,
        out_specs=(inside,) * 5,
        scratch_shapes=[
            pltpu.VMEM((blocks, tok, width), bf16),
            pltpu.VMEM((blocks, tok, width), bf16),
            pltpu.VMEM((blocks, experts, tok), f32),
            pltpu.VMEM((width, 2 * local * hidden), bf16),
            pltpu.VMEM((local * hidden, width), bf16),
            pltpu.VMEM((blocks, tok, 2 * local * hidden), bf16),
            pltpu.VMEM((blocks, tok, local * hidden), bf16),
            pltpu.VMEM((lines, tok, width), bf16),
            pltpu.VMEM((lines, tok, width), bf16),
            pltpu.VMEM((lines, side, tok, width), bf16),
            pltpu.VMEM((lines, side, tok, width), bf16),
            pltpu.VMEM((blocks, back_rows, tok), f32),
            pltpu.VMEM((blocks, back_rows, tok), f32),
            pltpu.VMEM((top, tok), jnp.int32),
            pltpu.VMEM((top, tok), jnp.int32),
            dma((2,)),
            dma((2,)),
            dma((3 * local,)),
            dma((lines, 2, 2)),
            dma((lines, rows, 2)),
            dma((blocks,)),
            dma((blocks,)),
            dma((blocks,)),
            dma((blocks,)),
            dma((lines, CUTS)),
            dma((lines, CUTS)),
            dma((lines, side, CUTS)),
            dma((lines, side, CUTS)),
            dma((blocks,)),
            dma((blocks,)),
        ],
        compiler_params=pltpu.CompilerParams(
            collective_id=0, has_side_effects=True, vmem_limit_bytes=limit
        ),
    )(
        jnp.swapaxes(expert_ids[0], 0, 1), jnp.swapaxes(route_levels[0], 0, 1),
        inputs[0], out_grads[0], w_gate[0], w_up[0], w_down[0],
    )
    upstream, own_routes, gates, ups, downs = pl.pallas_call(
        finish,
        out_shape=tuple(jax.ShapeDtypeStruct(shape, bf16) for shape in shapes),
        in_specs=[inside] * 5,
        out_specs=(anywhere,) * 5,
        scratch_shapes=[dma((5,))],
        compiler_params=pltpu.CompilerParams(vmem_limit_bytes=1_000_000),
    )(*[pltpu.with_memory_space_constraint(r, pltpu.VMEM) for r in results])
    token_route = jnp.swapaxes(own_routes, 0, 1)
    return (upstream[None], token_route[None], gates[None], ups[None], downs[None])


def solution(mesh):
    blocks = mesh.shape["expert"]
    rows = math.isqrt(max(blocks // 2, 1))
    while blocks % rows:
        rows -= 1
    in_specs = (
        P("section", "expert", None),
        P("section", "expert", None),
        P("section", "expert", None),
        P("section", "expert", None),
        P("section", "expert", None, None),
        P("section", "expert", None, None),
        P("section", "expert", None, None),
    )
    out_specs = (
        P("section", "expert", None),
        P("section", "expert", None),
        P("section", "expert", None, None),
        P("section", "expert", None, None),
        P("section", "expert", None, None),
    )
    return jax.shard_map(
        functools.partial(body, rows), mesh=mesh, in_specs=in_specs, out_specs=out_specs, check_vma=False
    )
```
